768 devices in a mesh: dp: 48 (over y_lo, z, core), section: 16 (over y_hi, x).
Axes of the slice: x: 4, y: 8 (y_hi: 4, y_lo: 2; y = y_hi * 2 + y_lo), z: 12, core: 2. Of those that a mesh axis runs over, the one named last changes fastest.
Arguments:
- hidden_act: bfloat16 [6144, 14336], P('dp', 'section'), may hold values from -6 to 6
- out_grad: bfloat16 [6144, 4608], P('dp'), may hold values from -0.076171875 to 0.076171875
- grad_accum: float32 [14336, 4608], P('section', 'dp'), may hold values from -6 to 6
- master_weight: float32 [14336, 4608], P('section', 'dp'), may hold values from -0.046875 to 0.046875
- adam_first: float32 [14336, 4608], P('section', 'dp'), may hold values from -2 to 2
- adam_second: float32 [14336, 4608], P('section', 'dp'), may hold values from 0.1 to 10
- decode_in: bfloat16 [4, 768, 14336], P(None, 'dp', 'section'), may hold values from -6 to 6
- residual_in: bfloat16 [4, 768, 4608], P(None, 'dp'), may hold values from -6 to 6
- norm_gain: bfloat16 [4608], P('section'), may hold values from 0.25 to 1.75
Outputs:
- weight_new: float32 [14336, 4608], P('section', 'dp')
- first_new: float32 [14336, 4608], P('section', 'dp')
- second_new: float32 [14336, 4608], P('section', 'dp')
- decoded: bfloat16 [4, 768, 4608], P(None, 'dp', 'section')
The draws below stay inside these ranges and needn't reach their ends.
All inputs are finite; a program needn't handle non-finite values.
Results may differ from the reference program's by a relative error of at most 0.0039.
Values may be sent and summed in bfloat16 or wider, within the bound.
A program may use at most 64 MiB of HBM per device.

```python
import math
import jax
import jax.numpy as jnp
from jax import lax

D = 4608
FF = 14336
STEPS = 4
TOKENS = 6144
ROLLOUT = 768


def spiked(values, rng, source, target, blocks, factor):
    owner, partner = [(jnp.arange(values.shape[position]) // (values.shape[position] // blocks)).reshape([-1 if axis == position else 1 for axis in range(values.ndim)]) for position in (source, target)]
    chosen = jax.random.permutation(rng, blocks)[partner]
    strong = (owner == chosen) | (owner == (partner + blocks // 2) % blocks)
    return jnp.where(strong, factor * values, values)


def shard_levels(own_key, dims, cuts, low, top_value):
    def one(axis_at, shards_of):
        steps = jax.random.uniform(jax.random.fold_in(jax.random.fold_in(own_key, 6), axis_at), (shards_of,), jnp.float32, low / len(cuts), top_value / len(cuts))
        return jnp.repeat(jnp.exp(steps), dims[axis_at] // shards_of).reshape((-1,) + (1,) * (len(dims) - axis_at - 1))

    loudness = one(*cuts[0])
    for cut in cuts[1:]:
        loudness = loudness * one(*cut)
    return loudness


def noise(own_key, shape, spread, limit, split=(), held_as=jnp.bfloat16):
    drawn = jax.random.normal(own_key, shape, jnp.float32) * spread
    if len(split) > 0:
        drawn = shard_levels(own_key, shape, split, -0.22, 0.18) * drawn
    return jnp.clip(drawn, min=-limit, max=limit).astype(held_as)


def noise_with(key, dims, deviation, most, pieces, heavy, kind=jnp.bfloat16):
    entries = deviation * jax.random.normal(key, dims, jnp.float32)
    if pieces:
        entries = entries * shard_levels(key, dims, pieces, -0.22, 0.18)
    return jnp.clip(spiked(entries, jax.random.fold_in(key, 3), *heavy), -most, most).astype(kind)


def setup_inputs(seed: int = 0) -> dict:
    streams_of = jax.random.split(jax.random.key(seed), 10)
    return {
        "hidden_act": noise(streams_of[0], (TOKENS, FF), 1.0, 6.0, ((0, 48), (1, 16))),
        "out_grad": noise_with(streams_of[1], (TOKENS, D), (TOKENS ** -0.5), 0.076171875, ((0, 48),), (0, 1, 48, 3.25)),
        "grad_accum": noise(streams_of[2], (FF, D), 1.0, 6.0, ((0, 16), (1, 48)), jnp.float32),
        "master_weight": noise(streams_of[3], (FF, D), FF ** -0.5, 0.046875, ((0, 16), (1, 48)), jnp.float32),
        "adam_first": noise(streams_of[4], (FF, D), 0.3, 2.0, ((0, 16), (1, 48)), jnp.float32),
        "adam_second": jnp.clip(jnp.exp(math.log(10.0) - 4.6051702 * jax.random.uniform(streams_of[5], (FF, D), jnp.float32) ** shard_levels(streams_of[5], (FF, D), ((0, 16), (1, 48)), -0.2, 0.2)), 0.1, 10.0),
        "decode_in": noise(streams_of[6], (STEPS, ROLLOUT, FF), 1.0, 6.0, ((1, 48), (2, 16))),
        "residual_in": noise(streams_of[7], (STEPS, ROLLOUT, D), 1.0, 6.0, ((1, 48),)),
        "norm_gain": jnp.clip(1.0 + 0.15 * jax.random.normal(streams_of[8], (D,), jnp.float32), 0.25, 1.75).astype(jnp.bfloat16),
    }


beta_first = 0.9
beta_second = 0.95
learn_rate = 0.002
decay_rate = 0.1
adam_eps = 1e-08
norm_eps = 1e-05
bias_first = 1.0 - 0.9 ** 10
bias_second = 1.0 - 0.95 ** 10

def reference(hidden_act, out_grad, grad_accum, master_weight, adam_first, adam_second, decode_in, residual_in, norm_gain):
    gradient = jnp.dot(hidden_act.T, out_grad, preferred_element_type=jnp.float32) + grad_accum
    first_new = beta_first * adam_first + (1.0 - beta_first) * gradient
    second_new = beta_second * adam_second + (1.0 - beta_second) * gradient * gradient
    update = first_new / bias_first / (jnp.sqrt(second_new / bias_second) + adam_eps)
    weight_new = master_weight - learn_rate * (update + decay_rate * master_weight)
    weight_rounded = weight_new.astype(jnp.bfloat16)
    flat_in = decode_in.reshape(STEPS * ROLLOUT, FF)
    stream = residual_in.reshape(STEPS * ROLLOUT, D).astype(jnp.float32) + jnp.dot(flat_in, weight_rounded, preferred_element_type=jnp.float32)
    mean_square = lax.optimization_barrier(jnp.mean(stream * stream, axis=1, keepdims=True))
    normed = stream * lax.rsqrt(mean_square + norm_eps) * norm_gain.astype(jnp.float32)
    decoded = normed.astype(jnp.bfloat16).reshape(STEPS, ROLLOUT, D)
    return (weight_new, first_new, second_new, decoded)
```

```python
import functools

import jax
import jax.numpy as jnp
from jax import lax
from jax.experimental import pallas as pl
from jax.experimental.pallas import tpu as pltpu
from jax.sharding import Mesh
from jax.sharding import PartitionSpec as P

DP = ("yl", "z", "c")
SECTION = ("yh", "x")
MESH_ID = pl.DeviceIdType.MESH

beta_first = 0.9
beta_second = 0.95
learn_rate = 0.002
decay_rate = 0.1
adam_eps = 1e-08
norm_eps = 1e-05
bias_first = 1.0 - 0.9**10
bias_second = 1.0 - 0.95**10


def remote(src, dst, send_sem, recv_sem, target):
    return pltpu.make_async_remote_copy(
        src_ref=src,
        dst_ref=dst,
        send_sem=send_sem,
        recv_sem=recv_sem,
        device_id=target,
        device_id_type=MESH_ID,
    )


def greet(targets):
    barrier = pltpu.get_barrier_semaphore()
    for target in targets:
        pl.semaphore_signal(barrier, inc=1, device_id=target, device_id_type=MESH_ID)
    pl.semaphore_wait(barrier, len(targets))


def grad_kernel(
    nz,
    h_ref,
    ot_ref,
    g_ref,
    hall,
    oall,
    part,
    sbuf,
    rbuf,
    h_send,
    h_recv,
    o_send,
    o_recv,
    r_send,
    r_recv,
):
    yl, z, c = lax.axis_index("yl"), lax.axis_index("z"), lax.axis_index("c")
    steps = nz // 2
    tokens, hidden = h_ref.shape
    rows = ot_ref.shape[3]
    half = rows // 2
    cut = (hidden // 256) * 128 + 128 if hidden > 128 else hidden
    lanes = [(0, cut), (cut, hidden - cut)] if hidden > cut else [(0, hidden)]
    core = {"c": 1 - c}
    across = {"yl": 1 - yl}
    diagonal = {"yl": 1 - yl, "c": 1 - c}
    up = {"z": lax.rem(z + 1, nz)}
    down = {"z": lax.rem(z + nz - 1, nz)}
    greet([core, across, diagonal, up, down])

    def h_copy(slot, src, target, index):
        return remote(
            src, hall.at[pl.ds(slot * tokens, tokens)], h_send.at[index], h_recv.at[index], target
        )

    h_across = h_copy(2, h_ref, across, 1)
    h_core = h_copy(1, h_ref, core, 0)
    h_forward = h_copy(3, hall.at[pl.ds(2 * tokens, tokens)], core, 2)
    h_across.start()
    h_core.start()

    def block_at(q):
        far = steps - (q + 1) // 2
        return lax.rem(jnp.where(q % 2 == 1, z + far, z + nz - far), nz)

    peers = [(1, core, yl, 1 - c), (2, across, 1 - yl, c), (3, diagonal, 1 - yl, 1 - c)]

    def o_copy(q, slot, target, to_yl, to_c):
        return remote(
            ot_ref.at[to_yl, block_at(q), to_c],
            oall.at[q, :, pl.ds(slot * tokens, tokens)],
            o_send.at[slot - 1, q],
            o_recv.at[slot - 1, q],
            target,
        )

    def send_blocks(q, carry):
        for peer in peers:
            o_copy(q, *peer).start()
        oall[q, :, pl.ds(0, tokens)] = ot_ref[yl, block_at(q), c]
        return carry

    lax.fori_loop(0, nz, send_blocks, 0)
    hall[pl.ds(0, tokens), :] = h_ref[...]
    h_across.wait_recv()
    h_forward.start()
    h_core.wait_recv()
    h_forward.wait_recv()

    def compute(q, slot, way):
        for peer in peers:
            o_copy(q, *peer).wait_recv()
        part[slot, way] = jnp.dot(oall[q], hall[...], preferred_element_type=jnp.float32)

    def r_copy(way, sub, n, t):
        first, width = lanes[n]
        spot = (way, sub, t, slice(None), pl.ds(first, width))
        return remote(
            sbuf.at[spot],
            rbuf.at[spot],
            r_send.at[way, sub, n, t],
            r_recv.at[way, sub, n, t],
            (up, down)[way],
        )

    def push(way, sub, n, t, slot, src_way, receive):
        first, width = lanes[n]
        value = part[slot, src_way, pl.ds(sub * half, half), pl.ds(first, width)]
        if receive:
            r_copy(way, sub, n, t - 1).wait_recv()
            value += rbuf[way, sub, t - 1, :, pl.ds(first, width)].astype(jnp.float32)
        sbuf[way, sub, t, :, pl.ds(first, width)] = value.astype(jnp.bfloat16)
        r_copy(way, sub, n, t).start()

    compute(0, 0, 0)
    for n in range(len(lanes)):
        push(0, 0, n, 0, 0, 0, False)
        push(1, 1, n, 0, 0, 0, False)

    def fill(t):
        slot = lax.rem(t, 2)
        compute(2 * t - 1, slot, 0)
        compute(2 * t, slot, 1)

    fill(1)
    for sub in range(2):
        for n in range(len(lanes)):
            push(0, sub, n, 1, 1, 0, sub == 0)
            push(1, 1 - sub, n, 1, 1, 1, sub == 0)

    def step(t, carry):
        fill(t)
        slot = lax.rem(t, 2)
        for sub in range(2):
            for n in range(len(lanes)):
                push(0, sub, n, t, slot, 0, True)
                push(1, 1 - sub, n, t, slot, 1, True)
        return carry

    lax.fori_loop(2, steps, step, 0)
    compute(nz - 1, 0, 0)
    for sub in range(2):
        for n, (first, width) in enumerate(lanes):
            value = part[0, 0, pl.ds(sub * half, half), pl.ds(first, width)]
            for way in range(2):
                r_copy(way, sub, n, steps - 1).wait_recv()
                value += rbuf[way, sub, steps - 1, :, pl.ds(first, width)].astype(jnp.float32)
            g_ref[pl.ds(sub * half, half), pl.ds(first, width)] = value

    h_across.wait_send()
    h_core.wait_send()
    h_forward.wait_send()

    def drain_blocks(q, carry):
        for peer in peers:
            o_copy(q, *peer).wait_send()
        return carry

    lax.fori_loop(0, nz, drain_blocks, 0)
    for n in range(len(lanes)):
        r_copy(0, 0, n, 0).wait_send()
        r_copy(1, 1, n, 0).wait_send()

    def drain(t, carry):
        for way in range(2):
            for sub in range(2):
                for n in range(len(lanes)):
                    r_copy(way, sub, n, t).wait_send()
        return carry

    lax.fori_loop(1, steps, drain, 0)


def gradient_share(nz, hidden_act, out_t):
    tokens, hidden = hidden_act.shape
    rows = out_t.shape[3]
    steps = nz // 2
    vmem = pl.BlockSpec(memory_space=pltpu.VMEM)
    return pl.pallas_call(
        functools.partial(grad_kernel, nz),
        out_shape=jax.ShapeDtypeStruct((rows, hidden), jnp.float32),
        in_specs=[vmem, vmem],
        out_specs=vmem,
        scratch_shapes=[
            pltpu.VMEM((4 * tokens, hidden), jnp.bfloat16),
            pltpu.VMEM((nz, rows, 4 * tokens), jnp.bfloat16),
            pltpu.VMEM((2, 2, rows, hidden), jnp.float32),
            pltpu.VMEM((2, 2, steps, rows // 2, hidden), jnp.bfloat16),
            pltpu.VMEM((2, 2, steps, rows // 2, hidden), jnp.bfloat16),
            pltpu.SemaphoreType.DMA((3,)),
            pltpu.SemaphoreType.DMA((3,)),
            pltpu.SemaphoreType.DMA((3, nz)),
            pltpu.SemaphoreType.DMA((3, nz)),
            pltpu.SemaphoreType.DMA((2, 2, 2, steps)),
            pltpu.SemaphoreType.DMA((2, 2, 2, steps)),
        ],
        compiler_params=pltpu.CompilerParams(collective_id=0, has_side_effects=True),
        cost_estimate=pl.CostEstimate(
            flops=2 * nz * rows * hidden * 4 * tokens, bytes_accessed=3000000, transcendentals=0
        ),
        name="gradient",
    )(hidden_act, out_t)


def decode_kernel(
    nz,
    w_ref,
    x_ref,
    resid_ref,
    gain_ref,
    out_ref,
    xb,
    wall,
    pbuf,
    xbuf,
    ysend,
    ybuf,
    ss_out,
    ss_in,
    p_send,
    p_recv,
    w_send,
    w_recv,
    c_send,
    c_recv,
    own_send,
    own_recv,
    x_send,
    x_recv,
    y_send,
    y_recv,
    s_send,
    s_recv,
):
    yl, z, c = lax.axis_index("yl"), lax.axis_index("z"), lax.axis_index("c")
    yh, x = lax.axis_index("yh"), lax.axis_index("x")
    steps = nz // 2
    cols, hidden = w_ref.shape
    half = cols // 2
    roll = x_ref.shape[0]
    per = 2 * nz // 8
    core = {"c": 1 - c}
    across = {"yl": 1 - yl}
    ring = ({"z": lax.rem(z + 1, nz)}, {"z": lax.rem(z + nz - 1, nz)})
    place = yh * 4 + x
    section = []
    for r in range(1, 16):
        other = lax.rem(place + r, 16)
        section.append({"yh": other // 4, "x": lax.rem(other, 4)})
    flipped = [{"yl": 1 - yl, "yh": other} for other in range(4)]
    greet([core, *ring, *section, *flipped])

    pair = remote(x_ref, xb.at[pl.ds(yl * roll, roll)], p_send.at[0], p_recv.at[0], across)
    own = remote(w_ref, wall.at[z, c], own_send.at[0], own_recv.at[0], core)

    def w_copy(way, sub, t, first=False):
        block = lax.rem(z + nz - t, nz) if way == 0 else lax.rem(z + t, nz)
        spot = wall.at[block, c, pl.ds(sub * half, half)]
        return remote(
            w_ref.at[pl.ds(sub * half, half)] if first else spot,
            spot,
            w_send.at[way, sub, t],
            w_recv.at[way, sub, t],
            ring[way],
        )

    def c_copy(way, sub, t):
        block = lax.rem(z + 2 * nz - 1 - t, nz) if way == 0 else lax.rem(z + 1 + t, nz)
        spot = wall.at[block, c, pl.ds(sub * half, half)]
        return remote(spot, spot, c_send.at[way, sub, t], c_recv.at[way, sub, t], core)

    for sub in range(2):
        for way in range(2):
            w_copy(way, sub, 0, True).start()
    own.start()
    pair.start()
    wall[z, c] = w_ref[...]
    xb[pl.ds(yl * roll, roll), :] = x_ref[...]
    pair.wait_recv()
    own.wait_recv()

    def x_copy(rel, j, k):
        return remote(
            pbuf.at[j, k],
            xbuf.at[rel - 1, j // 4, k],
            x_send.at[rel - 1, j // 4, k],
            x_recv.at[rel - 1, j // 4, k],
            {"x": lax.rem(x + rel, 4)},
        )

    def multiply(block):
        product = lax.dot_general(
            wall[block].reshape(2 * cols, hidden),
            xb[...],
            (((1,), (1,)), ((), ())),
            preferred_element_type=jnp.float32,
        )
        for lane in range(2):
            piece = 2 * block + lane
            j, k = piece // per, lax.rem(piece, per)
            pbuf[j, k] = product[lane * cols : (lane + 1) * cols].astype(jnp.bfloat16)
            rel = lax.rem(lax.rem(j, 4) + 4 - x, 4)

            @pl.when(rel != 0)
            def _():
                x_copy(rel, j, k).start()

    multiply(z)

    def pass_on(way, sub, t, last):
        w_copy(way, sub, t).wait_recv()
        if not last:
            w_copy(way, sub, t + 1).start()
        c_copy(way, sub, t).start()

    def step(t, carry):
        for way in range(2):
            pass_on(way, way, t, False)
        for way in range(2):
            w_copy(way, 1 - way, t).wait_recv()

            @pl.when(t < steps - 2)
            def _(way=way):
                w_copy(way, 1 - way, t + 1).start()

            c_copy(way, 1 - way, t).start()
        for way in range(2):
            for sub in range(2):
                c_copy(way, sub, t).wait_recv()
        multiply(lax.rem(z + nz - 1 - t, nz))
        multiply(lax.rem(z + 1 + t, nz))
        return carry

    lax.fori_loop(0, steps - 1, step, 0)
    for way in range(2):
        pass_on(way, way, steps - 1, True)
    for way in range(2):
        c_copy(way, way, steps - 1).wait_recv()
    multiply(lax.rem(z + steps, nz))

    def y_copy(to_yl, jj):
        return remote(
            ysend.at[to_yl, jj],
            ybuf.at[yh],
            y_send.at[to_yl, jj],
            y_recv.at[yh],
            {"yl": to_yl, "yh": 2 * yl + jj},
        )

    share = per * cols
    for jj in range(2):
        total = pbuf[jj * 4 + x].astype(jnp.float32)
        for rel in range(1, 4):
            for k in range(per):
                x_copy(rel, jj * 4, k).wait_recv()
            total += xbuf[rel - 1, jj].astype(jnp.float32)
        total = total.reshape(share, 2 * roll)
        for to_yl in range(2):
            rows = slice(to_yl * roll, (to_yl + 1) * roll)
            packed = jnp.concatenate(
                [total[: share // 2, rows], total[share // 2 :, rows]], axis=1
            ).astype(jnp.bfloat16)
            mine = jnp.logical_and(yl == to_yl, yh == 2 * yl + jj)

            @pl.when(mine)
            def _(packed=packed):
                ybuf[yh] = packed

            @pl.when(jnp.logical_not(mine))
            def _(packed=packed, to_yl=to_yl, jj=jj):
                ysend[to_yl, jj] = packed
                y_copy(to_yl, jj).start()

    stream = resid_ref[...]
    for source in range(4):
        mine = jnp.logical_and(yh == source, yh // 2 == yl)

        @pl.when(jnp.logical_not(mine))
        def _(source=source):
            remote(
                ysend.at[0, 0], ybuf.at[source], y_send.at[0, 0], y_recv.at[source], across
            ).wait_recv()

        stream += ybuf[source].astype(jnp.float32)

    square = jnp.sum(stream * stream, axis=0, keepdims=True)
    square = jnp.broadcast_to(square, (8, 2 * roll))
    square = square + pltpu.roll(square, roll, 1)
    ss_out[...] = square

    def s_copy(r):
        return remote(ss_out, ss_in.at[r - 1], s_send.at[r - 1], s_recv.at[r - 1], section[r - 1])

    for r in range(1, 16):
        s_copy(r).start()
    for r in range(1, 16):
        s_copy(r).wait_recv()
        square += ss_in[r - 1]
    scale = lax.rsqrt(square * (1.0 / (16 * share)) + norm_eps)
    out_ref[...] = (stream * scale[0:1] * gain_ref[...]).astype(jnp.bfloat16)

    pair.wait_send()
    own.wait_send()

    def drain(t, carry):
        for way in range(2):
            for sub in range(2):
                w_copy(way, sub, t).wait_send()
                c_copy(way, sub, t).wait_send()
        return carry

    lax.fori_loop(0, steps - 1, drain, 0)
    for way in range(2):
        w_copy(way, way, steps - 1).wait_send()
        c_copy(way, way, steps - 1).wait_send()
    for rel in range(1, 4):
        for jj in range(2):
            for k in range(per):
                x_copy(rel, jj * 4, k).wait_send()
    for jj in range(2):
        for to_yl in range(2):
            mine = jnp.logical_and(yl == to_yl, yh == 2 * yl + jj)

            @pl.when(jnp.logical_not(mine))
            def _(to_yl=to_yl, jj=jj):
                y_copy(to_yl, jj).wait_send()

    for r in range(1, 16):
        s_copy(r).wait_send()


def decode(nz, w, x, resid, gain):
    cols, hidden = w.shape
    roll = x.shape[0]
    steps = nz // 2
    per = 2 * nz // 8
    vmem = pl.BlockSpec(memory_space=pltpu.VMEM)
    dma = pltpu.SemaphoreType.DMA
    return pl.pallas_call(
        functools.partial(decode_kernel, nz),
        out_shape=jax.ShapeDtypeStruct(resid.shape, jnp.bfloat16),
        in_specs=[vmem] * 4,
        out_specs=vmem,
        scratch_shapes=[
            pltpu.VMEM((2 * roll, hidden), jnp.bfloat16),
            pltpu.VMEM((nz, 2, cols, hidden), jnp.bfloat16),
            pltpu.VMEM((8, per, cols, 2 * roll), jnp.bfloat16),
            pltpu.VMEM((3, 2, per, cols, 2 * roll), jnp.bfloat16),
            pltpu.VMEM((2, 2, *resid.shape), jnp.bfloat16),
            pltpu.VMEM((4, *resid.shape), jnp.bfloat16),
            pltpu.VMEM((8, 2 * roll), jnp.float32),
            pltpu.VMEM((15, 8, 2 * roll), jnp.float32),
            dma((1,)),
            dma((1,)),
            dma((2, 2, steps)),
            dma((2, 2, steps)),
            dma((2, 2, steps)),
            dma((2, 2, steps)),
            dma((1,)),
            dma((1,)),
            dma((3, 2, per)),
            dma((3, 2, per)),
            dma((2, 2)),
            dma((4,)),
            dma((15,)),
            dma((15,)),
        ],
        compiler_params=pltpu.CompilerParams(collective_id=1, has_side_effects=True),
        cost_estimate=pl.CostEstimate(
            flops=8 * nz * cols * hidden * roll, bytes_accessed=1000000, transcendentals=0
        ),
        name="decode",
    )(w, x, resid, gain)


def per_device(
    hidden_act,
    out_grad,
    grad_accum,
    master_weight,
    adam_first,
    adam_second,
    decode_in,
    residual_in,
    norm_gain,
):
    nz = lax.axis_size("z")
    tokens = hidden_act.shape[0]
    rows = master_weight.shape[1]
    out_t = out_grad.T.reshape(2, nz, 2, rows, tokens)
    grad_share = gradient_share(nz, hidden_act, out_t)
    gradient = grad_share.T + grad_accum
    first_new = beta_first * adam_first + (1.0 - beta_first) * gradient
    second_new = beta_second * adam_second + (1.0 - beta_second) * gradient * gradient
    update = first_new / bias_first / (jnp.sqrt(second_new / bias_second) + adam_eps)
    weight_new = master_weight - learn_rate * (update + decay_rate * master_weight)
    weight_rounded = weight_new.astype(jnp.bfloat16)
    steps_count, roll_rows, hidden_local = decode_in.shape
    flat_rows = steps_count * roll_rows
    flat_in = decode_in.reshape(flat_rows, hidden_local)
    share_width = norm_gain.shape[0]
    middle = share_width // 2
    resid_flat = residual_in.reshape(flat_rows, -1)
    offset = lax.axis_index(SECTION) * share_width
    resid = lax.dynamic_slice_in_dim(resid_flat, offset, share_width, 1)
    resid = resid.astype(jnp.float32).T
    resid = jnp.concatenate([resid[:middle], resid[middle:]], axis=1)
    gain = norm_gain.astype(jnp.float32).reshape(2, middle, 1)
    gain = jnp.broadcast_to(gain, (2, middle, flat_rows))
    gain = jnp.concatenate([gain[0], gain[1]], axis=1)
    packed = decode(nz, weight_rounded.T, flat_in, resid, gain)
    decoded = jnp.concatenate([packed[:, :flat_rows], packed[:, flat_rows:]], axis=0).T
    decoded = decoded.reshape(steps_count, roll_rows, share_width)
    return (weight_new, first_new, second_new, decoded)


def solution(mesh):
    finer = Mesh(mesh.devices.reshape(2, 12, 2, 4, 4), ("yl", "z", "c", "yh", "x"))
    in_specs = (
        P(DP, SECTION),
        P(DP, None),
        P(SECTION, DP),
        P(SECTION, DP),
        P(SECTION, DP),
        P(SECTION, DP),
        P(None, DP, SECTION),
        P(None, DP, None),
        P(SECTION),
    )
    out_specs = (P(SECTION, DP), P(SECTION, DP), P(SECTION, DP), P(None, DP, SECTION))
    return jax.shard_map(
        per_device, mesh=finer, in_specs=in_specs, out_specs=out_specs, check_vma=False
    )
```

```python
import functools

import jax
import jax.numpy as jnp
from jax import lax
from jax.experimental import pallas as pl
from jax.experimental.pallas import tpu as pltpu
from jax.sharding import Mesh
from jax.sharding import PartitionSpec as P

DP = ("yl", "z", "c")
SECTION = ("yh", "x")
MESH_ID = pl.DeviceIdType.MESH

beta_first = 0.9
beta_second = 0.95
learn_rate = 0.002
decay_rate = 0.1
adam_eps = 1e-08
norm_eps = 1e-05
bias_first = 1.0 - 0.9**10
bias_second = 1.0 - 0.95**10


def remote(src, dst, send_sem, recv_sem, target):
    return pltpu.make_async_remote_copy(
        src_ref=src,
        dst_ref=dst,
        send_sem=send_sem,
        recv_sem=recv_sem,
        device_id=target,
        device_id_type=MESH_ID,
    )


def greet(targets):
    barrier = pltpu.get_barrier_semaphore()
    for target in targets:
        pl.semaphore_signal(barrier, inc=1, device_id=target, device_id_type=MESH_ID)
    pl.semaphore_wait(barrier, len(targets))


def lane_cuts(hidden):
    if hidden < 256:
        return [(0, hidden)]
    cut = (hidden // 256) * 128 + 128 * ((hidden // 128) % 2)
    return [(0, cut), (cut, hidden - cut)]


def new_weight(gradient, master_weight, adam_first, adam_second):
    first_new = beta_first * adam_first + (1.0 - beta_first) * gradient
    second_new = beta_second * adam_second + (1.0 - beta_second) * gradient * gradient
    update = first_new / bias_first / (jnp.sqrt(second_new / bias_second) + adam_eps)
    weight_new = master_weight - learn_rate * (update + decay_rate * master_weight)
    return weight_new, first_new, second_new


def kernel(
    nz,
    h_ref,
    o_ref,
    x_ref,
    state_refs,
    resid_ref,
    g_ref,
    out_ref,
    ot,
    hall,
    oall,
    part,
    sbuf,
    rbuf,
    state,
    xb,
    wall,
    pbuf,
    xbuf,
    ysend,
    ybuf,
    ss_out,
    ss_in,
    window,
    turned,
    h_send,
    h_recv,
    o_send,
    o_recv,
    r_send,
    r_recv,
    local_sem,
    p_send,
    p_recv,
    w_send,
    w_recv,
    c_send,
    c_recv,
    own_send,
    own_recv,
    x_send,
    x_recv,
    y_send,
    y_recv,
    s_send,
    s_recv,
):
    yl, z, c = lax.axis_index("yl"), lax.axis_index("z"), lax.axis_index("c")
    yh, x = lax.axis_index("yh"), lax.axis_index("x")
    steps = nz // 2
    tokens, hidden = h_ref.shape
    cols = ot.shape[3]
    half = cols // 2
    roll = x_ref.shape[0]
    per = 2 * nz // 8
    share = per * cols
    lanes = lane_cuts(hidden)
    pieces = range(len(lanes))
    core = {"c": 1 - c}
    across = {"yl": 1 - yl}
    diagonal = {"yl": 1 - yl, "c": 1 - c}
    ring = ({"z": lax.rem(z + 1, nz)}, {"z": lax.rem(z + nz - 1, nz)})
    place = yh * 4 + x
    section = []
    for r in range(1, 16):
        other = lax.rem(place + r, 16)
        section.append({"yh": other // 4, "x": lax.rem(other, 4)})
    flipped = [{"yl": 1 - yl, "yh": other} for other in range(4)]

    loads = []
    for i, ref in enumerate(state_refs):
        loads.append(pltpu.make_async_copy(ref, state.at[i], local_sem.at[i]))
    for i in range(2):
        base = (place * share + i * (share // 2)) // 128 * 128
        loads.append(
            pltpu.make_async_copy(
                resid_ref.at[:, pl.ds(pl.multiple_of(base, 128), 256)],
                window.at[pl.ds(i * roll, roll)],
                local_sem.at[4 + i],
            )
        )
    for load in loads:
        load.start()
    greet([core, diagonal, *ring, *section, *flipped])

    def h_copy(slot, n):
        first, width = lanes[n]
        spot = hall.at[pl.ds(slot * tokens, tokens), pl.ds(first, width)]
        source = h_ref.at[:, pl.ds(first, width)]
        if slot == 3:
            source = hall.at[pl.ds(2 * tokens, tokens), pl.ds(first, width)]
        return remote(
            source,
            spot,
            h_send.at[slot - 1, n],
            h_recv.at[slot - 1, n],
            across if slot == 2 else core,
        )

    def block_at(q):
        far = steps - (q + 1) // 2
        return lax.rem(jnp.where(q % 2 == 1, z + far, z + nz - far), nz)

    peers = [(1, core, yl, 1 - c), (2, across, 1 - yl, c), (3, diagonal, 1 - yl, 1 - c)]

    def o_copy(q, slot, target, to_yl, to_c):
        return remote(
            ot.at[to_yl, block_at(q), to_c],
            oall.at[q, :, pl.ds(slot * tokens, tokens)],
            o_send.at[slot - 1, q],
            o_recv.at[slot - 1, q],
            target,
        )

    def send_blocks(q, carry):
        for peer in peers:
            o_copy(q, *peer).start()
        oall[q, :, pl.ds(0, tokens)] = ot[yl, block_at(q), c]
        return carry

    h_copy(2, 0).start()
    h_copy(1, 0).start()

    def turn(i, carry):
        block = o_ref[:, pl.ds(pl.multiple_of(i * 4 * cols, 128), 4 * cols)]
        block = block.astype(jnp.float32).T.astype(jnp.bfloat16)
        pair_at = pl.ds(lax.rem(i, steps) * 2, 2)
        ot[i // steps, pair_at] = block.reshape(2, 2, cols, tokens)
        return carry

    lax.fori_loop(0, nz, turn, 0)
    send_blocks(0, 0)
    for n in pieces[1:]:
        h_copy(2, n).start()
        h_copy(1, n).start()
    lax.fori_loop(1, nz, send_blocks, 0)
    pair = remote(x_ref, xb.at[pl.ds(yl * roll, roll)], p_send.at[0], p_recv.at[0], across)
    pair.start()
    hall[pl.ds(0, tokens), :] = h_ref[...]
    xb[pl.ds(yl * roll, roll), :] = x_ref[...]

    def compute(q, slot, way, n):
        first, width = lanes[n]
        part[slot, way, :, pl.ds(first, width)] = jnp.dot(
            oall[q], hall[:, pl.ds(first, width)], preferred_element_type=jnp.float32
        )

    def arrived(q):
        for peer in peers:
            o_copy(q, *peer).wait_recv()

    def r_copy(way, sub, n, t):
        first, width = lanes[n]
        spot = (way, sub, t, slice(None), pl.ds(first, width))
        return remote(
            sbuf.at[spot],
            rbuf.at[spot],
            r_send.at[way, sub, n, t],
            r_recv.at[way, sub, n, t],
            ring[way],
        )

    def push(way, sub, n, t, slot, src_way, receive):
        first, width = lanes[n]
        value = part[slot, src_way, pl.ds(sub * half, half), pl.ds(first, width)]
        if receive:
            r_copy(way, sub, n, t - 1).wait_recv()
            value += rbuf[way, sub, t - 1, :, pl.ds(first, width)].astype(jnp.float32)
        sbuf[way, sub, t, :, pl.ds(first, width)] = value.astype(jnp.bfloat16)
        r_copy(way, sub, n, t).start()

    for n in pieces:
        h_copy(2, n).wait_recv()
        h_copy(3, n).start()
        h_copy(1, n).wait_recv()
        h_copy(3, n).wait_recv()
        if n == 0:
            arrived(0)
        compute(0, 0, 0, n)
        push(0, 0, n, 0, 0, 0, False)
        push(1, 1, n, 0, 0, 0, False)

    def fill(t):
        slot = lax.rem(t, 2)
        for way in range(2):
            arrived(2 * t - 1 + way)
            for n in pieces:
                compute(2 * t - 1 + way, slot, way, n)

    fill(1)
    for sub in range(2):
        for n in pieces:
            push(0, sub, n, 1, 1, 0, sub == 0)
            push(1, 1 - sub, n, 1, 1, 1, sub == 0)

    def step(t, carry):
        fill(t)
        slot = lax.rem(t, 2)
        for sub in range(2):
            for n in pieces:
                push(0, sub, n, t, slot, 0, True)
                push(1, 1 - sub, n, t, slot, 1, True)
        return carry

    lax.fori_loop(2, steps, step, 0)

    for load in loads:
        load.wait()
    turned[...] = window[...].astype(jnp.float32).T
    arrived(nz - 1)
    for n in pieces:
        compute(nz - 1, 0, 0, n)

    def w_copy(way, sub, n, t):
        first, width = lanes[n]
        block = lax.rem(z + nz - t, nz) if way == 0 else lax.rem(z + t, nz)
        spot = wall.at[block, c, pl.ds(sub * half, half), pl.ds(first, width)]
        return remote(
            spot, spot, w_send.at[way, sub, n, t], w_recv.at[way, sub, n, t], ring[way]
        )

    def c_copy(way, sub, n, t):
        first, width = lanes[n]
        block = lax.rem(z + 2 * nz - 1 - t, nz) if way == 0 else lax.rem(z + 1 + t, nz)
        spot = wall.at[block, c, pl.ds(sub * half, half), pl.ds(first, width)]
        return remote(spot, spot, c_send.at[way, sub, n, t], c_recv.at[way, sub, n, t], core)

    def own_copy(sub, n):
        first, width = lanes[n]
        spot = wall.at[z, c, pl.ds(sub * half, half), pl.ds(first, width)]
        return remote(spot, spot, own_send.at[sub, n], own_recv.at[sub, n], core)

    for sub in range(2):
        for n in pieces:
            first, width = lanes[n]
            here = (pl.ds(sub * half, half), pl.ds(first, width))
            value = part[0, 0, here[0], here[1]]
            for way in range(2):
                r_copy(way, sub, n, steps - 1).wait_recv()
                value += rbuf[way, sub, steps - 1, :, here[1]].astype(jnp.float32)
            g_ref[here] = value
            value += state[0, here[0], here[1]]
            weight, _, _ = new_weight(
                value,
                state[1, here[0], here[1]],
                state[2, here[0], here[1]],
                state[3, here[0], here[1]],
            )
            wall[z, c, here[0], here[1]] = weight.astype(jnp.bfloat16)
            for way in range(2):
                w_copy(way, sub, n, 0).start()
            own_copy(sub, n).start()

    def x_copy(rel, j, k):
        return remote(
            pbuf.at[j, k],
            xbuf.at[rel - 1, j // 4, k],
            x_send.at[rel - 1, j // 4, k],
            x_recv.at[rel - 1, j // 4, k],
            {"x": lax.rem(x + rel, 4)},
        )

    def multiply(block):
        product = lax.dot_general(
            wall[block].reshape(2 * cols, hidden),
            xb[...],
            (((1,), (1,)), ((), ())),
            preferred_element_type=jnp.float32,
        )
        for lane in range(2):
            piece = 2 * block + lane
            j, k = piece // per, lax.rem(piece, per)
            pbuf[j, k] = product[lane * cols : (lane + 1) * cols].astype(jnp.bfloat16)
            rel = lax.rem(lax.rem(j, 4) + 4 - x, 4)

            @pl.when(rel != 0)
            def _():
                x_copy(rel, j, k).start()

    def pass_on(t, short):
        for sub in range(2):
            for n in pieces:
                for way in range(2):
                    if way == sub:
                        w_copy(way, sub, n, t).wait_recv()
                        if short is not None:
                            w_copy(way, sub, n, t + 1).start()
                        c_copy(way, sub, n, t).start()
                    elif short is not None:
                        w_copy(way, sub, n, t).wait_recv()
                        if short:
                            w_copy(way, sub, n, t + 1).start()
                        c_copy(way, sub, n, t).start()

    def multiply_step(t):
        for way in range(2):
            for sub in range(2):
                for n in pieces:
                    c_copy(way, sub, n, t).wait_recv()
            multiply(lax.rem(z + nz - 1 - t, nz) if way == 0 else lax.rem(z + 1 + t, nz))

    pair.wait_recv()
    pass_on(0, steps > 2)
    for sub in range(2):
        for n in pieces:
            own_copy(sub, n).wait_recv()
    multiply(z)

    def w_step(t, carry):
        pass_on(t, True)
        multiply_step(t - 1)
        return carry

    lax.fori_loop(1, steps - 2, w_step, 0)
    if steps > 2:
        pass_on(steps - 2, False)
        multiply_step(steps - 3)
    pass_on(steps - 1, None)
    multiply_step(steps - 2)
    for n in pieces:
        for way in range(2):
            c_copy(way, way, n, steps - 1).wait_recv()
    multiply(lax.rem(z + steps, nz))

    def y_copy(to_yl, jj):
        return remote(
            ysend.at[to_yl, jj],
            ybuf.at[yh],
            y_send.at[to_yl, jj],
            y_recv.at[yh],
            {"yl": to_yl, "yh": 2 * yl + jj},
        )

    for jj in range(2):
        total = pbuf[jj * 4 + x].astype(jnp.float32)
        for rel in range(1, 4):
            for k in range(per):
                x_copy(rel, jj * 4, k).wait_recv()
            total += xbuf[rel - 1, jj].astype(jnp.float32)
        total = total.reshape(share, 2 * roll)
        for to_yl in range(2):
            rows = slice(to_yl * roll, (to_yl + 1) * roll)
            packed = jnp.concatenate(
                [total[: share // 2, rows], total[share // 2 :, rows]], axis=1
            ).astype(jnp.bfloat16)
            mine = jnp.logical_and(yl == to_yl, yh == 2 * yl + jj)

            @pl.when(mine)
            def _(packed=packed):
                ybuf[yh] = packed

            @pl.when(jnp.logical_not(mine))
            def _(packed=packed, to_yl=to_yl, jj=jj):
                ysend[to_yl, jj] = packed
                y_copy(to_yl, jj).start()

    halves = []
    for i in range(2):
        shift = lax.rem(place * share + i * (share // 2), 128)
        halves.append(turned[pl.ds(pl.multiple_of(shift, 8), share // 2), :])
    lane_at = lax.broadcasted_iota(jnp.int32, (share // 2, 2 * roll), 1)
    stream = jnp.where(lane_at < roll, halves[0], halves[1])
    for source in range(4):
        mine = jnp.logical_and(yh == source, yh // 2 == yl)

        @pl.when(jnp.logical_not(mine))
        def _(source=source):
            remote(
                ysend.at[0, 0], ybuf.at[source], y_send.at[0, 0], y_recv.at[source], across
            ).wait_recv()

        stream += ybuf[source].astype(jnp.float32)

    square = jnp.sum(stream * stream, axis=0, keepdims=True)
    square = jnp.broadcast_to(square, (8, 2 * roll))
    square = square + pltpu.roll(square, roll, 1)
    ss_out[...] = square

    def s_copy(r):
        return remote(ss_out, ss_in.at[r - 1], s_send.at[r - 1], s_recv.at[r - 1], section[r - 1])

    for r in range(1, 16):
        s_copy(r).start()
    for r in range(1, 16):
        s_copy(r).wait_recv()
        square += ss_in[r - 1]
    scale = lax.rsqrt(square * (1.0 / (16 * share)) + norm_eps)
    out_ref[...] = stream * scale[0:1]

    pair.wait_send()
    for slot in range(1, 4):
        for n in pieces:
            h_copy(slot, n).wait_send()

    def drain_blocks(q, carry):
        for peer in peers:
            o_copy(q, *peer).wait_send()
        return carry

    lax.fori_loop(0, nz, drain_blocks, 0)
    for n in pieces:
        r_copy(0, 0, n, 0).wait_send()
        r_copy(1, 1, n, 0).wait_send()
        for sub in range(2):
            own_copy(sub, n).wait_send()
            w_copy(sub, sub, n, steps - 1).wait_send()
            c_copy(sub, sub, n, steps - 1).wait_send()

    def drain(t, carry):
        for way in range(2):
            for sub in range(2):
                for n in pieces:
                    r_copy(way, sub, n, t + 1).wait_send()
                    w_copy(way, sub, n, t).wait_send()
                    c_copy(way, sub, n, t).wait_send()
        return carry

    lax.fori_loop(0, steps - 1, drain, 0)
    for rel in range(1, 4):
        for jj in range(2):
            for k in range(per):
                x_copy(rel, jj * 4, k).wait_send()
    for jj in range(2):
        for to_yl in range(2):
            mine = jnp.logical_and(yl == to_yl, yh == 2 * yl + jj)

            @pl.when(jnp.logical_not(mine))
            def _(to_yl=to_yl, jj=jj):
                y_copy(to_yl, jj).wait_send()

    for r in range(1, 16):
        s_copy(r).wait_send()


def update_and_decode(nz, hidden_act, out_grad, flat_in, state, resid):
    tokens, hidden = hidden_act.shape
    cols = state[0].shape[0]
    roll = flat_in.shape[0]
    steps = nz // 2
    per = 2 * nz // 8
    middle = per * cols // 2
    vmem = pl.BlockSpec(memory_space=pltpu.VMEM)
    hbm = pl.BlockSpec(memory_space=pl.ANY)
    dma = pltpu.SemaphoreType.DMA
    links = [dma((2, 2, 2, steps))] * 2
    return pl.pallas_call(
        functools.partial(kernel, nz),
        out_shape=(
            jax.ShapeDtypeStruct((cols, hidden), jnp.float32),
            jax.ShapeDtypeStruct((middle, 2 * roll), jnp.float32),
        ),
        in_specs=[vmem, vmem, vmem, [hbm] * 4, hbm],
        out_specs=(vmem, vmem),
        scratch_shapes=[
            pltpu.VMEM((2, nz, 2, cols, tokens), jnp.bfloat16),
            pltpu.VMEM((4 * tokens, hidden), jnp.bfloat16),
            pltpu.VMEM((nz, cols, 4 * tokens), jnp.bfloat16),
            pltpu.VMEM((2, 2, cols, hidden), jnp.float32),
            pltpu.VMEM((2, 2, steps, cols // 2, hidden), jnp.bfloat16),
            pltpu.VMEM((2, 2, steps, cols // 2, hidden), jnp.bfloat16),
            pltpu.VMEM((4, cols, hidden), jnp.float32),
            pltpu.VMEM((2 * roll, hidden), jnp.bfloat16),
            pltpu.VMEM((nz, 2, cols, hidden), jnp.bfloat16),
            pltpu.VMEM((8, per, cols, 2 * roll), jnp.bfloat16),
            pltpu.VMEM((3, 2, per, cols, 2 * roll), jnp.bfloat16),
            pltpu.VMEM((2, 2, middle, 2 * roll), jnp.bfloat16),
            pltpu.VMEM((4, middle, 2 * roll), jnp.bfloat16),
            pltpu.VMEM((8, 2 * roll), jnp.float32),
            pltpu.VMEM((15, 8, 2 * roll), jnp.float32),
            pltpu.VMEM((2 * roll, 256), jnp.bfloat16),
            pltpu.VMEM((256, 2 * roll), jnp.float32),
            dma((3, 2)),
            dma((3, 2)),
            dma((3, nz)),
            dma((3, nz)),
            *links,
            dma((6,)),
            dma((1,)),
            dma((1,)),
            *links,
            *links,
            dma((2, 2)),
            dma((2, 2)),
            dma((3, 2, per)),
            dma((3, 2, per)),
            dma((2, 2)),
            dma((4,)),
            dma((15,)),
            dma((15,)),
        ],
        compiler_params=pltpu.CompilerParams(collective_id=0, has_side_effects=True),
        cost_estimate=pl.CostEstimate(
            flops=8 * nz * cols * hidden * (tokens + roll),
            bytes_accessed=3000000,
            transcendentals=0,
        ),
        name="update_and_decode",
    )(hidden_act, out_grad, flat_in, list(state), resid)


def per_device(
    hidden_act,
    out_grad,
    grad_accum,
    master_weight,
    adam_first,
    adam_second,
    decode_in,
    residual_in,
    norm_gain,
):
    nz = lax.axis_size("z")
    steps_count, roll_rows, hidden_local = decode_in.shape
    flat_rows = steps_count * roll_rows
    flat_in = decode_in.reshape(flat_rows, hidden_local)
    resid_flat = residual_in.reshape(flat_rows, -1)
    state = (grad_accum.T, master_weight.T, adam_first.T, adam_second.T)
    grad_share, packed = update_and_decode(
        nz, hidden_act, out_grad, flat_in, state, resid_flat
    )
    weight_new, first_new, second_new = new_weight(
        grad_share.T + grad_accum, master_weight, adam_first, adam_second
    )
    normed = jnp.concatenate([packed[:, :flat_rows], packed[:, flat_rows:]], axis=0).T
    decoded = (normed * norm_gain.astype(jnp.float32)).astype(jnp.bfloat16)
    decoded = decoded.reshape(steps_count, roll_rows, -1)
    return (weight_new, first_new, second_new, decoded)


def solution(mesh):
    finer = Mesh(mesh.devices.reshape(2, 12, 2, 4, 4), ("yl", "z", "c", "yh", "x"))
    in_specs = (
        P(DP, SECTION),
        P(DP, None),
        P(SECTION, DP),
        P(SECTION, DP),
        P(SECTION, DP),
        P(SECTION, DP),
        P(None, DP, SECTION),
        P(None, DP, None),
        P(SECTION),
    )
    out_specs = (P(SECTION, DP), P(SECTION, DP), P(SECTION, DP), P(None, DP, SECTION))
    return jax.shard_map(
        per_device, mesh=finer, in_specs=in_specs, out_specs=out_specs, check_vma=False
    )
```

```python
import functools

import jax
import jax.numpy as jnp
from jax import lax
from jax.experimental import pallas as pl
from jax.experimental.pallas import tpu as pltpu
from jax.sharding import Mesh
from jax.sharding import PartitionSpec as P

DP = ("yl", "z", "c")
SECTION = ("yh", "x")
MESH_ID = pl.DeviceIdType.MESH

beta_first = 0.9
beta_second = 0.95
learn_rate = 0.002
decay_rate = 0.1
adam_eps = 1e-08
norm_eps = 1e-05
bias_first = 1.0 - 0.9**10
bias_second = 1.0 - 0.95**10


def remote(src, dst, send_sem, recv_sem, target):
    return pltpu.make_async_remote_copy(
        src_ref=src,
        dst_ref=dst,
        send_sem=send_sem,
        recv_sem=recv_sem,
        device_id=target,
        device_id_type=MESH_ID,
    )


def greet(targets):
    barrier = pltpu.get_barrier_semaphore()
    for target in targets:
        pl.semaphore_signal(barrier, inc=1, device_id=target, device_id_type=MESH_ID)
    pl.semaphore_wait(barrier, len(targets))


def lane_cuts(hidden):
    if hidden < 256:
        return [(0, hidden)]
    cut = (hidden // 256) * 128
    return [(0, cut), (cut, hidden - cut)]


def new_weight(gradient, master_weight, adam_first, adam_second):
    first_new = beta_first * adam_first + (1.0 - beta_first) * gradient
    second_new = beta_second * adam_second + (1.0 - beta_second) * gradient * gradient
    update = first_new / bias_first / (jnp.sqrt(second_new / bias_second) + adam_eps)
    weight_new = master_weight - learn_rate * (update + decay_rate * master_weight)
    return weight_new, first_new, second_new


def kernel(
    nz,
    h_ref,
    o_ref,
    x_ref,
    state_refs,
    resid_ref,
    gain_ref,
    g_ref,
    out_ref,
    o_vm,
    ot,
    hall,
    oall,
    part,
    sbuf,
    rbuf,
    state,
    xb,
    wall,
    pbuf,
    xbuf,
    ysend,
    ybuf,
    ss_out,
    ss_in,
    window,
    turned,
    h_send,
    h_recv,
    o_send,
    o_recv,
    r_send,
    r_recv,
    local_sem,
    p_send,
    p_recv,
    w_send,
    w_recv,
    c_send,
    c_recv,
    own_send,
    own_recv,
    x_send,
    x_recv,
    y_send,
    y_recv,
    s_send,
    s_recv,
):
    yl, z, c = lax.axis_index("yl"), lax.axis_index("z"), lax.axis_index("c")
    yh, x = lax.axis_index("yh"), lax.axis_index("x")
    steps = nz // 2
    tokens, hidden = h_ref.shape
    cols = ot.shape[3]
    half = cols // 2
    roll = x_ref.shape[0]
    per = 2 * nz // 8
    share = per * cols
    lanes = lane_cuts(hidden)
    pieces = range(len(lanes))
    core = {"c": 1 - c}
    across = {"yl": 1 - yl}
    diagonal = {"yl": 1 - yl, "c": 1 - c}
    ring = ({"z": lax.rem(z + 1, nz)}, {"z": lax.rem(z + nz - 1, nz)})
    place = yh * 4 + x
    section = []
    for r in range(1, 16):
        other = lax.rem(place + r, 16)
        section.append({"yh": other // 4, "x": lax.rem(other, 4)})
    flipped = [{"yl": 1 - yl, "yh": other} for other in range(4)]

    width = o_ref.shape[1] // 3
    o_loads = []
    for i in range(3):
        part_at = (slice(None), pl.ds(i * width, width))
        o_loads.append(pltpu.make_async_copy(o_ref.at[part_at], o_vm.at[part_at], local_sem.at[6 + i]))
        o_loads[i].start()
    loads = []
    for i, ref in enumerate(state_refs):
        loads.append(pltpu.make_async_copy(ref, state.at[i], local_sem.at[i]))
    span = window.shape[1]
    shifts = []
    for i in range(2):
        first_col = place * share + i * half
        base = first_col // 128 * 128
        base = jnp.where(base > 16 * share - span, 16 * share - span, base)
        shifts.append(first_col - base)
        loads.append(
            pltpu.make_async_copy(
                resid_ref.at[:, pl.ds(pl.multiple_of(base, 128), span)],
                window.at[pl.ds(i * roll, roll)],
                local_sem.at[4 + i],
            )
        )
    for load in loads:
        load.start()
    greet([core, diagonal, *ring, *section, *flipped])

    def h_copy(slot, n):
        first, width = lanes[n]
        spot = hall.at[pl.ds(slot * tokens, tokens), pl.ds(first, width)]
        source = h_ref.at[:, pl.ds(first, width)]
        if slot == 3:
            source = hall.at[pl.ds(2 * tokens, tokens), pl.ds(first, width)]
        return remote(
            source,
            spot,
            h_send.at[slot - 1, n],
            h_recv.at[slot - 1, n],
            across if slot == 2 else core,
        )

    def block_at(q):
        far = steps - (q + 1) // 2
        return lax.rem(jnp.where(q % 2 == 1, z + far, z + nz - far), nz)

    peers = [(1, core, yl, 1 - c), (2, across, 1 - yl, c), (3, diagonal, 1 - yl, 1 - c)]

    def o_copy(q, slot, target, to_yl, to_c):
        return remote(
            ot.at[to_yl, block_at(q), to_c],
            oall.at[q, :, pl.ds(slot * tokens, tokens)],
            o_send.at[slot - 1, q],
            o_recv.at[slot - 1, q],
            target,
        )

    def send_blocks(q, carry):
        for peer in peers:
            o_copy(q, *peer).start()
        oall[q, :, pl.ds(0, tokens)] = ot[yl, block_at(q), c]
        return carry

    h_copy(2, 0).start()
    h_copy(1, 0).start()

    def turn(i, carry):
        block = o_vm[:, pl.ds(pl.multiple_of(i * 4 * cols, 128), 4 * cols)]
        block = block.astype(jnp.float32).T.astype(jnp.bfloat16)
        pair_at = pl.ds(lax.rem(i, steps) * 2, 2)
        ot[i // steps, pair_at] = block.reshape(2, 2, cols, tokens)
        return carry

    for i in range(3):
        o_loads[i].wait()
        lax.fori_loop(i * nz // 3, (i + 1) * nz // 3, turn, 0)
    send_blocks(0, 0)
    for n in pieces[1:]:
        h_copy(2, n).start()
        h_copy(1, n).start()
    lax.fori_loop(1, nz, send_blocks, 0)
    pair = remote(x_ref, xb.at[pl.ds(yl * roll, roll)], p_send.at[0], p_recv.at[0], across)
    pair.start()
    hall[pl.ds(0, tokens), :] = h_ref[...]
    xb[pl.ds(yl * roll, roll), :] = x_ref[...]

    def compute(q, slot, way, n):
        first, width = lanes[n]
        part[slot, way, :, pl.ds(first, width)] = jnp.dot(
            oall[q], hall[:, pl.ds(first, width)], preferred_element_type=jnp.float32
        )

    def arrived(q):
        for peer in peers:
            o_copy(q, *peer).wait_recv()

    def r_copy(way, sub, n, t):
        first, width = lanes[n]
        spot = (way, sub, t, slice(None), pl.ds(first, width))
        return remote(
            sbuf.at[spot],
            rbuf.at[spot],
            r_send.at[way, sub, n, t],
            r_recv.at[way, sub, n, t],
            ring[way],
        )

    def push(way, sub, n, t, slot, src_way, receive):
        first, width = lanes[n]
        value = part[slot, src_way, pl.ds(sub * half, half), pl.ds(first, width)]
        if receive:
            r_copy(way, sub, n, t - 1).wait_recv()
            value += rbuf[way, sub, t - 1, :, pl.ds(first, width)].astype(jnp.float32)
        sbuf[way, sub, t, :, pl.ds(first, width)] = value.astype(jnp.bfloat16)
        r_copy(way, sub, n, t).start()

    for n in pieces:
        h_copy(2, n).wait_recv()
        h_copy(3, n).start()
        h_copy(1, n).wait_recv()
        h_copy(3, n).wait_recv()
        if n == 0:
            arrived(0)
        compute(0, 0, 0, n)
        push(0, 0, n, 0, 0, 0, False)
        push(1, 1, n, 0, 0, 0, False)

    def fill(t):
        slot = lax.rem(t, 2)
        for way in range(2):
            arrived(2 * t - 1 + way)
            for n in pieces:
                compute(2 * t - 1 + way, slot, way, n)

    fill(1)
    for n in pieces:
        for sub in range(2):
            push(0, sub, n, 1, 1, 0, sub == 0)
            push(1, 1 - sub, n, 1, 1, 1, sub == 0)

    def step(t, carry):
        fill(t)
        slot = lax.rem(t, 2)
        for n in pieces:
            for sub in range(2):
                push(0, sub, n, t, slot, 0, True)
                push(1, 1 - sub, n, t, slot, 1, True)
        return carry

    lax.fori_loop(2, steps, step, 0)

    for load in loads:
        load.wait()
    turned[...] = window[...].astype(jnp.float32).T
    arrived(nz - 1)
    for n in pieces:
        compute(nz - 1, 0, 0, n)

    def w_copy(way, sub, n, t):
        first, width = lanes[n]
        block = lax.rem(z + nz - t, nz) if way == 0 else lax.rem(z + t, nz)
        spot = wall.at[block, c, pl.ds(sub * half, half), pl.ds(first, width)]
        return remote(
            spot, spot, w_send.at[way, sub, n, t], w_recv.at[way, sub, n, t], ring[way]
        )

    def c_copy(way, sub, n, t):
        first, width = lanes[n]
        block = lax.rem(z + 2 * nz - 1 - t, nz) if way == 0 else lax.rem(z + 1 + t, nz)
        spot = wall.at[block, c, pl.ds(sub * half, half), pl.ds(first, width)]
        return remote(spot, spot, c_send.at[way, sub, n, t], c_recv.at[way, sub, n, t], core)

    def own_copy(sub, n):
        first, width = lanes[n]
        spot = wall.at[z, c, pl.ds(sub * half, half), pl.ds(first, width)]
        return remote(spot, spot, own_send.at[sub, n], own_recv.at[sub, n], core)

    for n in pieces:
        for sub in range(2):
            first, width = lanes[n]
            here = (pl.ds(sub * half, half), pl.ds(first, width))
            value = part[0, 0, here[0], here[1]]
            for way in range(2):
                r_copy(way, sub, n, steps - 1).wait_recv()
                value += rbuf[way, sub, steps - 1, :, here[1]].astype(jnp.float32)
            g_ref[here] = value
            value += state[0, here[0], here[1]]
            weight, _, _ = new_weight(
                value,
                state[1, here[0], here[1]],
                state[2, here[0], here[1]],
                state[3, here[0], here[1]],
            )
            wall[z, c, here[0], here[1]] = weight.astype(jnp.bfloat16)
            for way in range(2):
                w_copy(way, sub, n, 0).start()
            own_copy(sub, n).start()

    def x_copy(rel, j, k):
        return remote(
            pbuf.at[j, k],
            xbuf.at[rel - 1, j // 4, k],
            x_send.at[rel - 1, j // 4, k],
            x_recv.at[rel - 1, j // 4, k],
            {"x": lax.rem(x + rel, 4)},
        )

    def multiply(block):
        product = lax.dot_general(
            wall[block].reshape(2 * cols, hidden),
            xb[...],
            (((1,), (1,)), ((), ())),
            preferred_element_type=jnp.float32,
        )
        for lane in range(2):
            piece = 2 * block + lane
            j, k = piece // per, lax.rem(piece, per)
            pbuf[j, k] = product[lane * cols : (lane + 1) * cols].astype(jnp.bfloat16)
            rel = lax.rem(lax.rem(j, 4) + 4 - x, 4)

            @pl.when(rel != 0)
            def _():
                x_copy(rel, j, k).start()

    def y_copy(to_yl, jj, k):
        return remote(
            ysend.at[to_yl, jj, k],
            ybuf.at[yh, k],
            y_send.at[to_yl, jj, k],
            y_recv.at[yh, k],
            {"yl": to_yl, "yh": 2 * yl + jj},
        )

    def finish(block):
        for lane in range(2):
            piece = 2 * block + lane
            j, k = piece // per, lax.rem(piece, per)
            jj = j // 4

            @pl.when(lax.rem(j, 4) == x)
            def _(j=j, k=k, jj=jj):
                total = pbuf[j, k].astype(jnp.float32)
                for rel in range(1, 4):
                    x_copy(rel, j, k).wait_recv()
                    total += xbuf[rel - 1, jj, k].astype(jnp.float32)
                for to_yl in range(2):
                    rows = slice(to_yl * roll, (to_yl + 1) * roll)
                    packed = jnp.concatenate(
                        [total[:half, rows], total[half:, rows]], axis=1
                    ).astype(jnp.bfloat16)
                    mine = jnp.logical_and(yl == to_yl, yh == 2 * yl + jj)

                    @pl.when(mine)
                    def _(packed=packed):
                        ybuf[yh, k] = packed

                    @pl.when(jnp.logical_not(mine))
                    def _(packed=packed, to_yl=to_yl):
                        ysend[to_yl, jj, k] = packed
                        y_copy(to_yl, jj, k).start()

    def finish_step(t):
        finish(lax.rem(z + nz - 1 - t, nz))
        finish(lax.rem(z + 1 + t, nz))

    def pass_on(t, short):
        for n in pieces:
            for sub in range(2):
                for way in range(2):
                    if way == sub:
                        w_copy(way, sub, n, t).wait_recv()
                        if short is not None:
                            w_copy(way, sub, n, t + 1).start()
                        c_copy(way, sub, n, t).start()
                    elif short is not None:
                        w_copy(way, sub, n, t).wait_recv()
                        if short:
                            w_copy(way, sub, n, t + 1).start()
                        c_copy(way, sub, n, t).start()

    def multiply_step(t):
        for way in range(2):
            for sub in range(2):
                for n in pieces:
                    c_copy(way, sub, n, t).wait_recv()
            multiply(lax.rem(z + nz - 1 - t, nz) if way == 0 else lax.rem(z + 1 + t, nz))

    pair.wait_recv()
    pass_on(0, steps > 2)
    for sub in range(2):
        for n in pieces:
            own_copy(sub, n).wait_recv()
    multiply(z)

    if steps > 3:
        pass_on(1, True)
        multiply_step(0)
        finish(z)

        def w_step(t, carry):
            pass_on(t, True)
            multiply_step(t - 1)
            finish_step(t - 2)
            return carry

        lax.fori_loop(2, steps - 2, w_step, 0)
        pass_on(steps - 2, False)
        multiply_step(steps - 3)
        finish_step(steps - 4)
        pass_on(steps - 1, None)
        multiply_step(steps - 2)
        finish_step(steps - 3)
    else:
        pass_on(steps - 1, None)
        multiply_step(steps - 2)
        finish(z)
    for n in pieces:
        for way in range(2):
            c_copy(way, way, n, steps - 1).wait_recv()
    multiply(lax.rem(z + steps, nz))
    finish_step(steps - 2)
    finish(lax.rem(z + steps, nz))

    lane_at = lax.broadcasted_iota(jnp.int32, (half, 2 * roll), 1)
    streams = []
    for k in range(per):
        left, right = [
            turned[pl.ds(pl.multiple_of(shift + k * cols, 8), half), :] for shift in shifts
        ]
        streams.append(jnp.where(lane_at < roll, left, right))
    for source in range(4):
        mine = jnp.logical_and(yh == source, yh // 2 == yl)

        @pl.when(jnp.logical_not(mine))
        def _(source=source):
            for k in range(per):
                remote(
                    ysend.at[0, 0, 0],
                    ybuf.at[source, k],
                    y_send.at[0, 0, 0],
                    y_recv.at[source, k],
                    across,
                ).wait_recv()

        for k in range(per):
            streams[k] += ybuf[source, k].astype(jnp.float32)
    stream = jnp.concatenate(streams, axis=0)

    square = jnp.sum(stream * stream, axis=0, keepdims=True)
    square = jnp.broadcast_to(square, (8, 2 * roll))
    square = square + pltpu.roll(square, roll, 1)
    ss_out[...] = square

    def s_copy(r):
        return remote(ss_out, ss_in.at[r - 1], s_send.at[r - 1], s_recv.at[r - 1], section[r - 1])

    for r in range(1, 16):
        s_copy(r).start()
    for r in range(1, 16):
        s_copy(r).wait_recv()
        square += ss_in[r - 1]
    scale = lax.rsqrt(square * (1.0 / (16 * share)) + norm_eps)
    normed = (stream * scale[0:1]).T
    natural = []
    for k in range(per):
        for i in range(2):
            natural.append(normed[i * roll : (i + 1) * roll, k * half : (k + 1) * half])
    natural = jnp.concatenate(natural, axis=1)
    out_ref[...] = (natural * gain_ref[...].astype(jnp.float32)).astype(jnp.bfloat16)

    pair.wait_send()
    for slot in range(1, 4):
        for n in pieces:
            h_copy(slot, n).wait_send()

    def drain_blocks(q, carry):
        for peer in peers:
            o_copy(q, *peer).wait_send()
        return carry

    lax.fori_loop(0, nz, drain_blocks, 0)
    for n in pieces:
        r_copy(0, 0, n, 0).wait_send()
        r_copy(1, 1, n, 0).wait_send()
        for sub in range(2):
            own_copy(sub, n).wait_send()
            w_copy(sub, sub, n, steps - 1).wait_send()
            c_copy(sub, sub, n, steps - 1).wait_send()

    def drain(t, carry):
        for way in range(2):
            for sub in range(2):
                for n in pieces:
                    r_copy(way, sub, n, t + 1).wait_send()
                    w_copy(way, sub, n, t).wait_send()
                    c_copy(way, sub, n, t).wait_send()
        return carry

    lax.fori_loop(0, steps - 1, drain, 0)
    for rel in range(1, 4):
        for jj in range(2):
            for k in range(per):
                x_copy(rel, jj * 4, k).wait_send()
    for jj in range(2):
        for to_yl in range(2):
            mine = jnp.logical_and(yl == to_yl, yh == 2 * yl + jj)

            @pl.when(jnp.logical_not(mine))
            def _(to_yl=to_yl, jj=jj):
                for k in range(per):
                    y_copy(to_yl, jj, k).wait_send()

    for r in range(1, 16):
        s_copy(r).wait_send()


def update_and_decode(nz, hidden_act, out_grad, flat_in, state, resid, gain):
    tokens, hidden = hidden_act.shape
    cols = state[0].shape[0]
    roll = flat_in.shape[0]
    steps = nz // 2
    per = 2 * nz // 8
    half = cols // 2
    share = per * cols
    span = (2 * cols + half + 112 + 127) // 128 * 128
    vmem = pl.BlockSpec(memory_space=pltpu.VMEM)
    hbm = pl.BlockSpec(memory_space=pl.ANY)
    dma = pltpu.SemaphoreType.DMA
    links = [dma((2, 2, 2, steps))] * 2
    return pl.pallas_call(
        functools.partial(kernel, nz),
        out_shape=(
            jax.ShapeDtypeStruct((cols, hidden), jnp.float32),
            jax.ShapeDtypeStruct((roll, share), jnp.bfloat16),
        ),
        in_specs=[vmem, hbm, vmem, [hbm] * 4, hbm, vmem],
        out_specs=(vmem, vmem),
        scratch_shapes=[
            pltpu.VMEM(out_grad.shape, jnp.bfloat16),
            pltpu.VMEM((2, nz, 2, cols, tokens), jnp.bfloat16),
            pltpu.VMEM((4 * tokens, hidden), jnp.bfloat16),
            pltpu.VMEM((nz, cols, 4 * tokens), jnp.bfloat16),
            pltpu.VMEM((2, 2, cols, hidden), jnp.float32),
            pltpu.VMEM((2, 2, steps, cols // 2, hidden), jnp.bfloat16),
            pltpu.VMEM((2, 2, steps, cols // 2, hidden), jnp.bfloat16),
            pltpu.VMEM((4, cols, hidden), jnp.float32),
            pltpu.VMEM((2 * roll, hidden), jnp.bfloat16),
            pltpu.VMEM((nz, 2, cols, hidden), jnp.bfloat16),
            pltpu.VMEM((8, per, cols, 2 * roll), jnp.bfloat16),
            pltpu.VMEM((3, 2, per, cols, 2 * roll), jnp.bfloat16),
            pltpu.VMEM((2, 2, per, half, 2 * roll), jnp.bfloat16),
            pltpu.VMEM((4, per, half, 2 * roll), jnp.bfloat16),
            pltpu.VMEM((8, 2 * roll), jnp.float32),
            pltpu.VMEM((15, 8, 2 * roll), jnp.float32),
            pltpu.VMEM((2 * roll, span), jnp.bfloat16),
            pltpu.VMEM((span, 2 * roll), jnp.float32),
            dma((3, 2)),
            dma((3, 2)),
            dma((3, nz)),
            dma((3, nz)),
            *links,
            dma((9,)),
            dma((1,)),
            dma((1,)),
            *links,
            *links,
            dma((2, 2)),
            dma((2, 2)),
            dma((3, 2, per)),
            dma((3, 2, per)),
            dma((2, 2, per)),
            dma((4, per)),
            dma((15,)),
            dma((15,)),
        ],
        compiler_params=pltpu.CompilerParams(collective_id=0, has_side_effects=True),
        cost_estimate=pl.CostEstimate(
            flops=8 * nz * cols * hidden * (tokens + roll),
            bytes_accessed=3000000,
            transcendentals=0,
        ),
        name="update_and_decode",
    )(hidden_act, out_grad, flat_in, list(state), resid, gain)


def per_device(
    hidden_act,
    out_grad,
    grad_accum,
    master_weight,
    adam_first,
    adam_second,
    decode_in,
    residual_in,
    norm_gain,
):
    nz = lax.axis_size("z")
    steps_count, roll_rows, hidden_local = decode_in.shape
    flat_rows = steps_count * roll_rows
    flat_in = decode_in.reshape(flat_rows, hidden_local)
    resid_flat = residual_in.reshape(flat_rows, -1)
    state = (grad_accum.T, master_weight.T, adam_first.T, adam_second.T)
    grad_share, decoded = update_and_decode(
        nz, hidden_act, out_grad, flat_in, state, resid_flat, norm_gain[None]
    )
    weight_new, first_new, second_new = new_weight(
        grad_share.T + grad_accum, master_weight, adam_first, adam_second
    )
    decoded = decoded.reshape(steps_count, roll_rows, -1)
    return (weight_new, first_new, second_new, decoded)


def solution(mesh):
    finer = Mesh(mesh.devices.reshape(2, 12, 2, 4, 4), ("yl", "z", "c", "yh", "x"))
    in_specs = (
        P(DP, SECTION),
        P(DP, None),
        P(SECTION, DP),
        P(SECTION, DP),
        P(SECTION, DP),
        P(SECTION, DP),
        P(None, DP, SECTION),
        P(None, DP, None),
        P(SECTION),
    )
    out_specs = (P(SECTION, DP), P(SECTION, DP), P(SECTION, DP), P(None, DP, SECTION))
    return jax.shard_map(
        per_device, mesh=finer, in_specs=in_specs, out_specs=out_specs, check_vma=False
    )
```

```python
import functools

import jax
import jax.numpy as jnp
from jax import lax
from jax.experimental import pallas as pl
from jax.experimental.pallas import tpu as pltpu
from jax.sharding import Mesh
from jax.sharding import PartitionSpec as P

DP = ("yl", "z", "c")
SECTION = ("yh", "x")
MESH_ID = pl.DeviceIdType.MESH

beta_first = 0.9
beta_second = 0.95
learn_rate = 0.002
decay_rate = 0.1
adam_eps = 1e-08
norm_eps = 1e-05
bias_first = 1.0 - 0.9**10
bias_second = 1.0 - 0.95**10


def remote(src, dst, send_sem, recv_sem, target):
    return pltpu.make_async_remote_copy(
        src_ref=src,
        dst_ref=dst,
        send_sem=send_sem,
        recv_sem=recv_sem,
        device_id=target,
        device_id_type=MESH_ID,
    )


def greet(targets):
    barrier = pltpu.get_barrier_semaphore()
    for target in targets:
        pl.semaphore_signal(barrier, inc=1, device_id=target, device_id_type=MESH_ID)
    pl.semaphore_wait(barrier, len(targets))


def lane_cuts(hidden):
    if hidden < 256:
        return [(0, hidden)]
    cut = (hidden // 256) * 128
    return [(0, cut), (cut, hidden - cut)]


def new_weight(gradient, master_weight, adam_first, adam_second):
    first_new = beta_first * adam_first + (1.0 - beta_first) * gradient
    second_new = beta_second * adam_second + (1.0 - beta_second) * gradient * gradient
    update = first_new / bias_first / (jnp.sqrt(second_new / bias_second) + adam_eps)
    weight_new = master_weight - learn_rate * (update + decay_rate * master_weight)
    return weight_new, first_new, second_new


def kernel(
    nz,
    h_ref,
    o_ref,
    x_ref,
    state_refs,
    resid_ref,
    g_ref,
    out_ref,
    h_vm,
    x_vm,
    o_vm,
    ot,
    hall,
    oall,
    part,
    sbuf,
    rbuf,
    state,
    xb,
    wall,
    pbuf,
    xbuf,
    ysend,
    ybuf,
    ss_out,
    ss_in,
    window,
    turned,
    h_send,
    h_recv,
    o_send,
    o_recv,
    r_send,
    r_recv,
    local_sem,
    p_send,
    p_recv,
    w_send,
    w_recv,
    c_send,
    c_recv,
    own_send,
    own_recv,
    x_send,
    x_recv,
    y_send,
    y_recv,
    s_send,
    s_recv,
):
    yl, z, c = lax.axis_index("yl"), lax.axis_index("z"), lax.axis_index("c")
    yh, x = lax.axis_index("yh"), lax.axis_index("x")
    steps = nz // 2
    tokens, hidden = h_ref.shape
    cols = ot.shape[3]
    half = cols // 2
    roll = x_ref.shape[0]
    per = 2 * nz // 8
    share = per * cols
    lanes = lane_cuts(hidden)
    pieces = range(len(lanes))
    core = {"c": 1 - c}
    across = {"yl": 1 - yl}
    diagonal = {"yl": 1 - yl, "c": 1 - c}
    ring = ({"z": lax.rem(z + 1, nz)}, {"z": lax.rem(z + nz - 1, nz)})
    place = yh * 4 + x
    section = []
    for r in range(1, 16):
        other = lax.rem(place + r, 16)
        section.append({"yh": other // 4, "x": lax.rem(other, 4)})
    flipped = [{"yl": 1 - yl, "yh": other} for other in range(4)]

    h_load = pltpu.make_async_copy(h_ref, h_vm, local_sem.at[9])
    x_load = pltpu.make_async_copy(x_ref, x_vm, local_sem.at[10])
    h_load.start()
    width = o_ref.shape[1] // 3
    o_loads = []
    for i in range(3):
        part_at = (slice(None), pl.ds(i * width, width))
        o_loads.append(pltpu.make_async_copy(o_ref.at[part_at], o_vm.at[part_at], local_sem.at[6 + i]))
        o_loads[i].start()
    x_load.start()
    loads = []
    for i, ref in enumerate(state_refs):
        loads.append(pltpu.make_async_copy(ref, state.at[i], local_sem.at[i]))
    span = window.shape[1]
    shifts = []
    for i in range(2):
        first_col = place * share + i * half
        base = first_col // 128 * 128
        base = jnp.where(base > 16 * share - span, 16 * share - span, base)
        shifts.append(first_col - base)
        loads.append(
            pltpu.make_async_copy(
                resid_ref.at[:, pl.ds(pl.multiple_of(base, 128), span)],
                window.at[pl.ds(i * roll, roll)],
                local_sem.at[4 + i],
            )
        )
    for load in loads:
        load.start()
    greet([core, diagonal, *ring, *section, *flipped])

    def h_copy(slot, n):
        first, width = lanes[n]
        spot = hall.at[pl.ds(slot * tokens, tokens), pl.ds(first, width)]
        source = h_vm.at[:, pl.ds(first, width)]
        if slot == 3:
            source = hall.at[pl.ds(2 * tokens, tokens), pl.ds(first, width)]
        return remote(
            source,
            spot,
            h_send.at[slot - 1, n],
            h_recv.at[slot - 1, n],
            across if slot == 2 else core,
        )

    def block_at(q):
        far = steps - (q + 1) // 2
        return lax.rem(jnp.where(q % 2 == 1, z + far, z + nz - far), nz)

    peers = [(1, core, yl, 1 - c), (2, across, 1 - yl, c), (3, diagonal, 1 - yl, 1 - c)]

    def o_copy(q, slot, target, to_yl, to_c):
        return remote(
            ot.at[to_yl, block_at(q), to_c],
            oall.at[q, :, pl.ds(slot * tokens, tokens)],
            o_send.at[slot - 1],
            o_recv.at[q],
            target,
        )

    def send_blocks(q, carry):
        for peer in peers:
            o_copy(q, *peer).start()
        oall[q, :, pl.ds(0, tokens)] = ot[yl, block_at(q), c]
        return carry

    h_load.wait()
    h_copy(2, 0).start()
    h_copy(1, 0).start()

    def turn(i, carry):
        block = o_vm[:, pl.ds(pl.multiple_of(i * 4 * cols, 128), 4 * cols)]
        block = block.astype(jnp.float32).T.astype(jnp.bfloat16)
        pair_at = pl.ds(lax.rem(i, steps) * 2, 2)
        ot[i // steps, pair_at] = block.reshape(2, 2, cols, tokens)
        return carry

    for i in range(3):
        o_loads[i].wait()
        lax.fori_loop(i * nz // 3, (i + 1) * nz // 3, turn, 0)
    send_blocks(0, 0)
    for n in pieces[1:]:
        h_copy(2, n).start()
        h_copy(1, n).start()
    lax.fori_loop(1, nz, send_blocks, 0)
    x_load.wait()
    pair = remote(x_vm, xb.at[pl.ds(yl * roll, roll)], p_send.at[0], p_recv.at[0], across)
    pair.start()
    hall[pl.ds(0, tokens), :] = h_vm[...]
    xb[pl.ds(yl * roll, roll), :] = x_vm[...]

    def compute(q, slot, way, n):
        first, width = lanes[n]
        part[slot, way, :, pl.ds(first, width)] = jnp.dot(
            oall[q], hall[:, pl.ds(first, width)], preferred_element_type=jnp.float32
        )

    def arrived(q):
        spot = oall.at[q, :, pl.ds(tokens, 3 * tokens)]
        remote(spot, spot, o_send.at[0], o_recv.at[q], core).wait_recv()

    def r_copy(way, sub, n, t):
        first, width = lanes[n]
        spot = (way, sub, t, slice(None), pl.ds(first, width))
        return remote(
            sbuf.at[spot],
            rbuf.at[spot],
            r_send.at[way, sub],
            r_recv.at[way, sub, n, t],
            ring[way],
        )

    def push(way, sub, n, t, slot, src_way, receive):
        first, width = lanes[n]
        value = part[slot, src_way, pl.ds(sub * half, half), pl.ds(first, width)]
        if receive:
            r_copy(way, sub, n, t - 1).wait_recv()
            value += rbuf[way, sub, t - 1, :, pl.ds(first, width)].astype(jnp.float32)
        sbuf[way, sub, t, :, pl.ds(first, width)] = value.astype(jnp.bfloat16)
        r_copy(way, sub, n, t).start()

    for n in pieces:
        h_copy(2, n).wait_recv()
        h_copy(3, n).start()
        h_copy(1, n).wait_recv()
        h_copy(3, n).wait_recv()
        if n == 0:
            arrived(0)
        compute(0, 0, 0, n)
        push(0, 0, n, 0, 0, 0, False)
        push(1, 1, n, 0, 0, 0, False)

    def fill(t):
        slot = lax.rem(t, 2)
        for way in range(2):
            arrived(2 * t - 1 + way)
            for n in pieces:
                compute(2 * t - 1 + way, slot, way, n)

    fill(1)
    for n in pieces:
        for sub in range(2):
            push(0, sub, n, 1, 1, 0, sub == 0)
            push(1, 1 - sub, n, 1, 1, 1, sub == 0)

    def step(t, carry):
        fill(t)
        slot = lax.rem(t, 2)
        for n in pieces:
            for sub in range(2):
                push(0, sub, n, t, slot, 0, True)
                push(1, 1 - sub, n, t, slot, 1, True)
        return carry

    lax.fori_loop(2, steps, step, 0)

    for load in loads:
        load.wait()
    turned[...] = window[...].astype(jnp.float32).T
    arrived(nz - 1)
    for n in pieces:
        compute(nz - 1, 0, 0, n)

    def w_copy(way, sub, n, t):
        first, width = lanes[n]
        block = lax.rem(z + nz - t, nz) if way == 0 else lax.rem(z + t, nz)
        spot = wall.at[block, c, pl.ds(sub * half, half), pl.ds(first, width)]
        return remote(
            spot, spot, w_send.at[way, sub], w_recv.at[way, sub, n, t], ring[way]
        )

    def c_copy(way, sub, n, t):
        first, width = lanes[n]
        block = lax.rem(z + 2 * nz - 1 - t, nz) if way == 0 else lax.rem(z + 1 + t, nz)
        spot = wall.at[block, c, pl.ds(sub * half, half), pl.ds(first, width)]
        return remote(spot, spot, c_send.at[way, sub], c_recv.at[way, t], core)

    def own_copy(sub, n):
        first, width = lanes[n]
        spot = wall.at[z, c, pl.ds(sub * half, half), pl.ds(first, width)]
        return remote(spot, spot, own_send.at[0], own_recv.at[0], core)

    for n in pieces:
        for sub in range(2):
            first, width = lanes[n]
            here = (pl.ds(sub * half, half), pl.ds(first, width))
            value = part[0, 0, here[0], here[1]]
            for way in range(2):
                r_copy(way, sub, n, steps - 1).wait_recv()
                value += rbuf[way, sub, steps - 1, :, here[1]].astype(jnp.float32)
            g_ref[here] = value
            value += state[0, here[0], here[1]]
            weight, _, _ = new_weight(
                value,
                state[1, here[0], here[1]],
                state[2, here[0], here[1]],
                state[3, here[0], here[1]],
            )
            wall[z, c, here[0], here[1]] = weight.astype(jnp.bfloat16)
            for way in range(2):
                w_copy(way, sub, n, 0).start()
            own_copy(sub, n).start()

    def x_copy(rel, j, k):
        return remote(
            pbuf.at[j, k],
            xbuf.at[rel - 1, j // 4, k],
            x_send.at[rel - 1],
            x_recv.at[j // 4, k],
            {"x": lax.rem(x + rel, 4)},
        )

    def multiply(block):
        product = lax.dot_general(
            wall[block].reshape(2 * cols, hidden),
            xb[...],
            (((1,), (1,)), ((), ())),
            preferred_element_type=jnp.float32,
        )
        for lane in range(2):
            piece = 2 * block + lane
            j, k = piece // per, lax.rem(piece, per)
            pbuf[j, k] = product[lane * cols : (lane + 1) * cols].astype(jnp.bfloat16)
            rel = lax.rem(lax.rem(j, 4) + 4 - x, 4)

            @pl.when(rel != 0)
            def _():
                x_copy(rel, j, k).start()

    def y_copy(to_yl, jj, k):
        return remote(
            ysend.at[to_yl, jj, k],
            ybuf.at[yh, k],
            y_send.at[to_yl, jj],
            y_recv.at[yh],
            {"yl": to_yl, "yh": 2 * yl + jj},
        )

    def finish(block):
        for lane in range(2):
            piece = 2 * block + lane
            j, k = piece // per, lax.rem(piece, per)
            jj = j // 4

            @pl.when(lax.rem(j, 4) == x)
            def _(j=j, k=k, jj=jj):
                total = pbuf[j, k].astype(jnp.float32)
                spot = xbuf.at[:, jj, k]
                remote(spot, spot, x_send.at[0], x_recv.at[jj, k], core).wait_recv()
                for rel in range(1, 4):
                    total += xbuf[rel - 1, jj, k].astype(jnp.float32)
                for to_yl in range(2):
                    rows = slice(to_yl * roll, (to_yl + 1) * roll)
                    packed = jnp.concatenate(
                        [total[:half, rows], total[half:, rows]], axis=1
                    ).astype(jnp.bfloat16)
                    mine = jnp.logical_and(yl == to_yl, yh == 2 * yl + jj)

                    @pl.when(mine)
                    def _(packed=packed):
                        ybuf[yh, k] = packed

                    @pl.when(jnp.logical_not(mine))
                    def _(packed=packed, to_yl=to_yl):
                        ysend[to_yl, jj, k] = packed
                        y_copy(to_yl, jj, k).start()

    def finish_step(t):
        finish(lax.rem(z + nz - 1 - t, nz))
        finish(lax.rem(z + 1 + t, nz))

    def pass_on(t, short):
        for n in pieces:
            for sub in range(2):
                for way in range(2):
                    if way == sub:
                        w_copy(way, sub, n, t).wait_recv()
                        if short is not None:
                            w_copy(way, sub, n, t + 1).start()
                        c_copy(way, sub, n, t).start()
                    elif short is not None:
                        w_copy(way, sub, n, t).wait_recv()
                        if short:
                            w_copy(way, sub, n, t + 1).start()
                        c_copy(way, sub, n, t).start()

    def multiply_step(t):
        for way in range(2):
            block = lax.rem(z + nz - 1 - t, nz) if way == 0 else lax.rem(z + 1 + t, nz)
            spot = wall.at[block, 1 - c]
            remote(spot, spot, c_send.at[0, 0], c_recv.at[way, t], core).wait_recv()
            multiply(block)

    pair.wait_recv()
    pass_on(0, steps > 2)
    remote(wall.at[0, 0], wall.at[z, 1 - c], own_send.at[0], own_recv.at[0], core).wait_recv()
    multiply(z)

    if steps > 3:
        pass_on(1, True)
        multiply_step(0)
        finish(z)

        def w_step(t, carry):
            pass_on(t, True)
            multiply_step(t - 1)
            finish_step(t - 2)
            return carry

        lax.fori_loop(2, steps - 2, w_step, 0)
        pass_on(steps - 2, False)
        multiply_step(steps - 3)
        finish_step(steps - 4)
        pass_on(steps - 1, None)
        multiply_step(steps - 2)
        finish_step(steps - 3)
    else:
        pass_on(steps - 1, None)
        multiply_step(steps - 2)
        finish(z)
    for way in range(2):
        spot = wall.at[lax.rem(z + steps, nz), 1 - c, pl.ds(way * half, half)]
        remote(spot, spot, c_send.at[0, 0], c_recv.at[way, steps - 1], core).wait_recv()
    multiply(lax.rem(z + steps, nz))
    finish_step(steps - 2)
    finish(lax.rem(z + steps, nz))

    lane_at = lax.broadcasted_iota(jnp.int32, (half, 2 * roll), 1)
    streams = []
    for k in range(per):
        left, right = [
            turned[pl.ds(pl.multiple_of(shift + k * cols, 8), half), :] for shift in shifts
        ]
        streams.append(jnp.where(lane_at < roll, left, right))
    for source in range(4):
        mine = jnp.logical_and(yh == source, yh // 2 == yl)

        @pl.when(jnp.logical_not(mine))
        def _(source=source):
            remote(
                ysend.at[0, 0], ybuf.at[source], y_send.at[0, 0], y_recv.at[source], across
            ).wait_recv()

        for k in range(per):
            streams[k] += ybuf[source, k].astype(jnp.float32)
    stream = jnp.concatenate(streams, axis=0)

    square = jnp.sum(stream * stream, axis=0, keepdims=True)
    square = jnp.broadcast_to(square, (8, 2 * roll))
    square = square + pltpu.roll(square, roll, 1)
    ss_out[...] = square

    def s_copy(r):
        return remote(ss_out, ss_in.at[r - 1], s_send.at[0], s_recv.at[0], section[r - 1])

    for r in range(1, 16):
        s_copy(r).start()
    remote(ss_in, ss_in, s_send.at[0], s_recv.at[0], core).wait_recv()
    for r in range(1, 16):
        square += ss_in[r - 1]
    scale = lax.rsqrt(square * (1.0 / (16 * share)) + norm_eps)
    normed = (stream * scale[0:1]).T
    natural = []
    for k in range(per):
        for i in range(2):
            natural.append(normed[i * roll : (i + 1) * roll, k * half : (k + 1) * half])
    natural = jnp.concatenate(natural, axis=1)
    out_ref[...] = natural

    pair.wait_send()
    for slot in range(1, 4):
        for n in pieces:
            h_copy(slot, n).wait_send()

    def drain(ref, sem):
        remote(ref, ref, sem, p_recv.at[0], core).wait_send()

    for slot in range(3):
        drain(ot.at[0, :, 0], o_send.at[slot])
        drain(xbuf.at[slot], x_send.at[slot])
    drain(wall.at[0, 0], own_send.at[0])
    for way in range(2):
        for sub in range(2):
            count = steps if way == sub else steps - 1
            for sem in (r_send, w_send, c_send):
                drain(sbuf.at[way, sub, pl.ds(0, count)], sem.at[way, sub])
    for jj in range(2):
        for to_yl in range(2):
            mine = jnp.logical_and(yl == to_yl, yh == 2 * yl + jj)

            @pl.when(jnp.logical_not(mine))
            def _(to_yl=to_yl, jj=jj):
                spot = ysend.at[to_yl, jj]
                remote(spot, spot, y_send.at[to_yl, jj], y_recv.at[0], across).wait_send()

    drain(ss_in, s_send.at[0])


def update_and_decode(nz, hidden_act, out_grad, flat_in, state, resid):
    tokens, hidden = hidden_act.shape
    cols = state[0].shape[0]
    roll = flat_in.shape[0]
    steps = nz // 2
    per = 2 * nz // 8
    half = cols // 2
    share = per * cols
    span = (2 * cols + half + 112 + 127) // 128 * 128
    vmem = pl.BlockSpec(memory_space=pltpu.VMEM)
    hbm = pl.BlockSpec(memory_space=pl.ANY)
    dma = pltpu.SemaphoreType.DMA
    return pl.pallas_call(
        functools.partial(kernel, nz),
        out_shape=(
            jax.ShapeDtypeStruct((cols, hidden), jnp.float32),
            jax.ShapeDtypeStruct((roll, share), jnp.float32),
        ),
        in_specs=[hbm, hbm, hbm, [hbm] * 4, hbm],
        out_specs=(vmem, vmem),
        scratch_shapes=[
            pltpu.VMEM(hidden_act.shape, jnp.bfloat16),
            pltpu.VMEM(flat_in.shape, jnp.bfloat16),
            pltpu.VMEM(out_grad.shape, jnp.bfloat16),
            pltpu.VMEM((2, nz, 2, cols, tokens), jnp.bfloat16),
            pltpu.VMEM((4 * tokens, hidden), jnp.bfloat16),
            pltpu.VMEM((nz, cols, 4 * tokens), jnp.bfloat16),
            pltpu.VMEM((2, 2, cols, hidden), jnp.float32),
            pltpu.VMEM((2, 2, steps, cols // 2, hidden), jnp.bfloat16),
            pltpu.VMEM((2, 2, steps, cols // 2, hidden), jnp.bfloat16),
            pltpu.VMEM((4, cols, hidden), jnp.float32),
            pltpu.VMEM((2 * roll, hidden), jnp.bfloat16),
            pltpu.VMEM((nz, 2, cols, hidden), jnp.bfloat16),
            pltpu.VMEM((8, per, cols, 2 * roll), jnp.bfloat16),
            pltpu.VMEM((3, 2, per, cols, 2 * roll), jnp.bfloat16),
            pltpu.VMEM((2, 2, per, half, 2 * roll), jnp.bfloat16),
            pltpu.VMEM((4, per, half, 2 * roll), jnp.bfloat16),
            pltpu.VMEM((8, 2 * roll), jnp.float32),
            pltpu.VMEM((15, 8, 2 * roll), jnp.float32),
            pltpu.VMEM((2 * roll, span), jnp.bfloat16),
            pltpu.VMEM((span, 2 * roll), jnp.float32),
            dma((3, 2)),
            dma((3, 2)),
            dma((3,)),
            dma((nz,)),
            dma((2, 2)),
            dma((2, 2, 2, steps)),
            dma((11,)),
            dma((1,)),
            dma((1,)),
            dma((2, 2)),
            dma((2, 2, 2, steps)),
            dma((2, 2)),
            dma((2, steps)),
            dma((1,)),
            dma((1,)),
            dma((3,)),
            dma((2, per)),
            dma((2, 2)),
            dma((4,)),
            dma((1,)),
            dma((1,)),
        ],
        compiler_params=pltpu.CompilerParams(collective_id=0, has_side_effects=True),
        cost_estimate=pl.CostEstimate(
            flops=8 * nz * cols * hidden * (tokens + roll),
            bytes_accessed=3000000,
            transcendentals=0,
        ),
        name="update_and_decode",
    )(hidden_act, out_grad, flat_in, list(state), resid)


def per_device(
    hidden_act,
    out_grad,
    grad_accum,
    master_weight,
    adam_first,
    adam_second,
    decode_in,
    residual_in,
    norm_gain,
):
    nz = lax.axis_size("z")
    steps_count, roll_rows, hidden_local = decode_in.shape
    flat_rows = steps_count * roll_rows
    flat_in = decode_in.reshape(flat_rows, hidden_local)
    resid_flat = residual_in.reshape(flat_rows, -1)
    state = (grad_accum.T, master_weight.T, adam_first.T, adam_second.T)
    grad_share, normed = update_and_decode(
        nz, hidden_act, out_grad, flat_in, state, resid_flat
    )
    weight_new, first_new, second_new = new_weight(
        grad_share.T + grad_accum, master_weight, adam_first, adam_second
    )
    decoded = (normed * norm_gain.astype(jnp.float32)).astype(jnp.bfloat16)
    decoded = decoded.reshape(steps_count, roll_rows, -1)
    return (weight_new, first_new, second_new, decoded)


def solution(mesh):
    finer = Mesh(mesh.devices.reshape(2, 12, 2, 4, 4), ("yl", "z", "c", "yh", "x"))
    in_specs = (
        P(DP, SECTION),
        P(DP, None),
        P(SECTION, DP),
        P(SECTION, DP),
        P(SECTION, DP),
        P(SECTION, DP),
        P(None, DP, SECTION),
        P(None, DP, None),
        P(SECTION),
    )
    out_specs = (P(SECTION, DP), P(SECTION, DP), P(SECTION, DP), P(None, DP, SECTION))
    return jax.shard_map(
        per_device, mesh=finer, in_specs=in_specs, out_specs=out_specs, check_vma=False
    )
```

```python
import functools

import jax
import jax.numpy as jnp
from jax import lax
from jax.experimental import pallas as pl
from jax.experimental.pallas import tpu as pltpu
from jax.sharding import Mesh
from jax.sharding import PartitionSpec as P

DP = ("yl", "z", "c")
SECTION = ("yh", "x")
MESH_ID = pl.DeviceIdType.MESH

beta_first = 0.9
beta_second = 0.95
learn_rate = 0.002
decay_rate = 0.1
adam_eps = 1e-08
norm_eps = 1e-05
bias_first = 1.0 - 0.9**10
bias_second = 1.0 - 0.95**10


def remote(src, dst, send_sem, recv_sem, target):
    return pltpu.make_async_remote_copy(
        src_ref=src,
        dst_ref=dst,
        send_sem=send_sem,
        recv_sem=recv_sem,
        device_id=target,
        device_id_type=MESH_ID,
    )


def greet(targets):
    barrier = pltpu.get_barrier_semaphore()
    for target in targets:
        pl.semaphore_signal(barrier, inc=1, device_id=target, device_id_type=MESH_ID)
    pl.semaphore_wait(barrier, len(targets))


def lane_cuts(hidden):
    if hidden < 256:
        return [(0, hidden)]
    cut = (hidden // 256) * 128
    return [(0, cut), (cut, hidden - cut)]


def new_weight(gradient, master_weight, adam_first, adam_second):
    first_new = beta_first * adam_first + (1.0 - beta_first) * gradient
    second_new = beta_second * adam_second + (1.0 - beta_second) * gradient * gradient
    update = first_new / bias_first / (jnp.sqrt(second_new / bias_second) + adam_eps)
    weight_new = master_weight - learn_rate * (update + decay_rate * master_weight)
    return weight_new, first_new, second_new


def kernel(
    nz,
    h_ref,
    o_ref,
    x_ref,
    state_refs,
    resid_ref,
    g_ref,
    out_ref,
    h_vm,
    x_vm,
    o_vm,
    ot,
    hall,
    oall,
    part,
    sbuf,
    rbuf,
    state,
    xb,
    wall,
    pbuf,
    xbuf,
    ysend,
    ybuf,
    ss_out,
    ss_in,
    window,
    turned,
    h_send,
    h_recv,
    o_send,
    o_recv,
    r_send,
    r_recv,
    local_sem,
    p_send,
    p_recv,
    w_send,
    w_recv,
    c_send,
    c_recv,
    own_send,
    own_recv,
    x_send,
    x_recv,
    y_send,
    y_recv,
    s_send,
    s_recv,
):
    yl, z, c = lax.axis_index("yl"), lax.axis_index("z"), lax.axis_index("c")
    yh, x = lax.axis_index("yh"), lax.axis_index("x")
    steps = nz // 2
    tokens, hidden = h_ref.shape
    cols = ot.shape[3]
    half = cols // 2
    roll = x_ref.shape[0]
    per = 2 * nz // 8
    share = per * cols
    lanes = lane_cuts(hidden)
    pieces = range(len(lanes))
    core = {"c": 1 - c}
    across = {"yl": 1 - yl}
    diagonal = {"yl": 1 - yl, "c": 1 - c}
    ring = ({"z": lax.rem(z + 1, nz)}, {"z": lax.rem(z + nz - 1, nz)})
    place = yh * 4 + x
    section = []
    for r in range(1, 16):
        other = lax.rem(place + r, 16)
        section.append({"yh": other // 4, "x": lax.rem(other, 4)})
    flipped = [{"yl": 1 - yl, "yh": other} for other in range(4)]

    h_load = pltpu.make_async_copy(h_ref, h_vm, local_sem.at[9])
    x_load = pltpu.make_async_copy(x_ref, x_vm, local_sem.at[10])
    h_load.start()
    width = o_ref.shape[1] // 3
    o_loads = []
    for i in range(3):
        part_at = (slice(None), pl.ds(i * width, width))
        o_loads.append(pltpu.make_async_copy(o_ref.at[part_at], o_vm.at[part_at], local_sem.at[6 + i]))
        o_loads[i].start()
    x_load.start()
    loads = []
    for i, ref in enumerate(state_refs):
        loads.append(pltpu.make_async_copy(ref, state.at[i], local_sem.at[i]))
    span = window.shape[1]
    shifts = []
    for i in range(2):
        first_col = place * share + i * half
        base = first_col // 128 * 128
        base = jnp.where(base > 16 * share - span, 16 * share - span, base)
        shifts.append(first_col - base)
        loads.append(
            pltpu.make_async_copy(
                resid_ref.at[:, pl.ds(pl.multiple_of(base, 128), span)],
                window.at[pl.ds(i * roll, roll)],
                local_sem.at[4 + i],
            )
        )
    for load in loads:
        load.start()
    greet([core, diagonal, *ring, *section, *flipped])

    def h_copy(slot, n):
        first, width = lanes[n]
        spot = hall.at[pl.ds(slot * tokens, tokens), pl.ds(first, width)]
        source = h_vm.at[:, pl.ds(first, width)]
        if slot == 3:
            source = hall.at[pl.ds(2 * tokens, tokens), pl.ds(first, width)]
        return remote(
            source,
            spot,
            h_send.at[slot - 1, n],
            h_recv.at[slot - 1, n],
            across if slot == 2 else core,
        )

    def block_at(q):
        far = steps - (q + 1) // 2
        return lax.rem(jnp.where(q % 2 == 1, z + far, z + nz - far), nz)

    peers = [(1, core, yl, 1 - c), (2, across, 1 - yl, c), (3, diagonal, 1 - yl, 1 - c)]

    def o_copy(q, slot, target, to_yl, to_c):
        return remote(
            ot.at[to_yl, block_at(q), to_c],
            oall.at[q, :, pl.ds(slot * tokens, tokens)],
            o_send.at[slot - 1],
            o_recv.at[q],
            target,
        )

    def send_blocks(q, carry):
        for peer in peers:
            o_copy(q, *peer).start()
        oall[q, :, pl.ds(0, tokens)] = ot[yl, block_at(q), c]
        return carry

    h_load.wait()
    h_copy(2, 0).start()
    h_copy(1, 0).start()

    def turn(i, carry):
        block = o_vm[:, pl.ds(pl.multiple_of(i * 4 * cols, 128), 4 * cols)]
        block = block.astype(jnp.float32).T.astype(jnp.bfloat16)
        pair_at = pl.ds(lax.rem(i, steps) * 2, 2)
        ot[i // steps, pair_at] = block.reshape(2, 2, cols, tokens)
        return carry

    for i in range(3):
        o_loads[i].wait()
        lax.fori_loop(i * nz // 3, (i + 1) * nz // 3, turn, 0)
    send_blocks(0, 0)
    for n in pieces[1:]:
        h_copy(2, n).start()
        h_copy(1, n).start()
    lax.fori_loop(1, nz, send_blocks, 0)
    x_load.wait()
    pair = remote(x_vm, xb.at[pl.ds(yl * roll, roll)], p_send.at[0], p_recv.at[0], across)
    pair.start()
    hall[pl.ds(0, tokens), :] = h_vm[...]
    xb[pl.ds(yl * roll, roll), :] = x_vm[...]

    def compute(q, slot, way, n):
        first, width = lanes[n]
        part[slot, way, :, pl.ds(first, width)] = jnp.dot(
            oall[q], hall[:, pl.ds(first, width)], preferred_element_type=jnp.float32
        )

    def arrived(q):
        spot = oall.at[q, :, pl.ds(tokens, 3 * tokens)]
        remote(spot, spot, o_send.at[0], o_recv.at[q], core).wait_recv()

    def r_copy(way, sub, n, t):
        first, width = lanes[n]
        spot = (way, sub, t, slice(None), pl.ds(first, width))
        return remote(
            sbuf.at[spot],
            rbuf.at[spot],
            r_send.at[way, sub],
            r_recv.at[way, sub, n, t],
            ring[way],
        )

    def push(way, sub, n, t, slot, src_way, receive):
        first, width = lanes[n]
        value = part[slot, src_way, pl.ds(sub * half, half), pl.ds(first, width)]
        if receive:
            r_copy(way, sub, n, t - 1).wait_recv()
            value += rbuf[way, sub, t - 1, :, pl.ds(first, width)].astype(jnp.float32)
        sbuf[way, sub, t, :, pl.ds(first, width)] = value.astype(jnp.bfloat16)
        r_copy(way, sub, n, t).start()

    def first_push(n):
        h_copy(2, n).wait_recv()
        h_copy(3, n).start()
        h_copy(1, n).wait_recv()
        h_copy(3, n).wait_recv()
        if n == 0:
            arrived(0)
        compute(0, 0, 0, n)
        push(0, 0, n, 0, 0, 0, False)
        push(1, 1, n, 0, 0, 0, False)

    def fill(t, n):
        slot = lax.rem(t, 2)
        for way in range(2):
            if n == 0:
                arrived(2 * t - 1 + way)
            compute(2 * t - 1 + way, slot, way, n)

    def push_all(n, t, receive=True):
        slot = lax.rem(t, 2)
        for sub in range(2):
            push(0, sub, n, t, slot, 0, receive or sub == 0)
            push(1, 1 - sub, n, t, slot, 1, receive or sub == 0)

    first_push(0)
    fill(1, 0)
    for n in pieces[1:]:
        first_push(n)
    push_all(0, 1, False)
    for n in pieces[1:]:
        fill(1, n)
    fill(2, 0)
    push_all(0, 2)
    for n in pieces[1:]:
        push_all(n, 1, False)

    def step(t, carry):
        fill(t, 0)
        for n in pieces[1:]:
            fill(t - 1, n)
        push_all(0, t)
        for n in pieces[1:]:
            push_all(n, t - 1)
        return carry

    lax.fori_loop(3, steps, step, 0)
    for n in pieces[1:]:
        fill(steps - 1, n)

    for load in loads:
        load.wait()
    turned[...] = window[...].astype(jnp.float32).T
    arrived(nz - 1)
    for n in pieces:
        compute(nz - 1, steps % 2, 0, n)

    def w_copy(way, sub, n, t):
        first, width = lanes[n]
        block = lax.rem(z + nz - t, nz) if way == 0 else lax.rem(z + t, nz)
        spot = wall.at[block, c, pl.ds(sub * half, half), pl.ds(first, width)]
        return remote(
            spot, spot, w_send.at[way, sub], w_recv.at[way, sub, n, t], ring[way]
        )

    def c_copy(way, sub, n, t):
        first, width = lanes[n]
        block = lax.rem(z + 2 * nz - 1 - t, nz) if way == 0 else lax.rem(z + 1 + t, nz)
        spot = wall.at[block, c, pl.ds(sub * half, half), pl.ds(first, width)]
        return remote(spot, spot, c_send.at[way, sub], c_recv.at[way, t], core)

    def own_copy(sub, n):
        first, width = lanes[n]
        spot = wall.at[z, c, pl.ds(sub * half, half), pl.ds(first, width)]
        return remote(spot, spot, own_send.at[0], own_recv.at[0], core)

    def settle(n):
        for sub in range(2):
            first, width = lanes[n]
            here = (pl.ds(sub * half, half), pl.ds(first, width))
            value = part[steps % 2, 0, here[0], here[1]]
            for way in range(2):
                r_copy(way, sub, n, steps - 1).wait_recv()
                value += rbuf[way, sub, steps - 1, :, here[1]].astype(jnp.float32)
            g_ref[here] = value
            value += state[0, here[0], here[1]]
            weight, _, _ = new_weight(
                value,
                state[1, here[0], here[1]],
                state[2, here[0], here[1]],
                state[3, here[0], here[1]],
            )
            wall[z, c, here[0], here[1]] = weight.astype(jnp.bfloat16)
            for way in range(2):
                w_copy(way, sub, n, 0).start()
            own_copy(sub, n).start()

    def x_copy(rel, j, k):
        return remote(
            pbuf.at[j, k],
            xbuf.at[rel - 1, j // 4, k],
            x_send.at[rel - 1],
            x_recv.at[j // 4, k],
            {"x": lax.rem(x + rel, 4)},
        )

    def multiply(block):
        product = lax.dot_general(
            wall[block].reshape(2 * cols, hidden),
            xb[...],
            (((1,), (1,)), ((), ())),
            preferred_element_type=jnp.float32,
        )
        for lane in range(2):
            piece = 2 * block + lane
            j, k = piece // per, lax.rem(piece, per)
            pbuf[j, k] = product[lane * cols : (lane + 1) * cols].astype(jnp.bfloat16)
            rel = lax.rem(lax.rem(j, 4) + 4 - x, 4)

            @pl.when(rel != 0)
            def _():
                x_copy(rel, j, k).start()

    def y_copy(to_yl, jj, k):
        return remote(
            ysend.at[to_yl, jj, k],
            ybuf.at[yh, k],
            y_send.at[to_yl, jj],
            y_recv.at[yh],
            {"yl": to_yl, "yh": 2 * yl + jj},
        )

    def finish(block):
        for lane in range(2):
            piece = 2 * block + lane
            j, k = piece // per, lax.rem(piece, per)
            jj = j // 4

            @pl.when(lax.rem(j, 4) == x)
            def _(j=j, k=k, jj=jj):
                total = pbuf[j, k].astype(jnp.float32)
                spot = xbuf.at[:, jj, k]
                remote(spot, spot, x_send.at[0], x_recv.at[jj, k], core).wait_recv()
                for rel in range(1, 4):
                    total += xbuf[rel - 1, jj, k].astype(jnp.float32)
                for to_yl in range(2):
                    rows = slice(to_yl * roll, (to_yl + 1) * roll)
                    packed = jnp.concatenate(
                        [total[:half, rows], total[half:, rows]], axis=1
                    ).astype(jnp.bfloat16)
                    mine = jnp.logical_and(yl == to_yl, yh == 2 * yl + jj)

                    @pl.when(mine)
                    def _(packed=packed):
                        ybuf[yh, k] = packed

                    @pl.when(jnp.logical_not(mine))
                    def _(packed=packed, to_yl=to_yl):
                        ysend[to_yl, jj, k] = packed
                        y_copy(to_yl, jj, k).start()

    def finish_step(t):
        finish(lax.rem(z + nz - 1 - t, nz))
        finish(lax.rem(z + 1 + t, nz))

    def pass_on(n, t):
        for sub in range(2):
            for way in range(2):
                last = steps - 1 if way == sub else steps - 2
                if t <= last:
                    w_copy(way, sub, n, t).wait_recv()
                    if t < last:
                        w_copy(way, sub, n, t + 1).start()
                    c_copy(way, sub, n, t).start()

    def multiply_step(t):
        for way in range(2):
            block = lax.rem(z + nz - 1 - t, nz) if way == 0 else lax.rem(z + 1 + t, nz)
            spot = wall.at[block, 1 - c]
            remote(spot, spot, c_send.at[0, 0], c_recv.at[way, t], core).wait_recv()
            multiply(block)

    settle(0)
    for n in pieces[1:]:
        push_all(n, steps - 1)
    pass_on(0, 0)
    for n in pieces[1:]:
        settle(n)
    pair.wait_recv()
    for t in range(steps):
        if t < steps - 1:
            pass_on(0, t + 1)
        for n in pieces[1:]:
            pass_on(n, t)
        if t == 0:
            remote(
                wall.at[0, 0], wall.at[z, 1 - c], own_send.at[0], own_recv.at[0], core
            ).wait_recv()
            multiply(z)
        else:
            multiply_step(t - 1)
        if t == 1:
            finish(z)
        if t > 1:
            finish_step(t - 2)
    for way in range(2):
        spot = wall.at[lax.rem(z + steps, nz), 1 - c, pl.ds(way * half, half)]
        remote(spot, spot, c_send.at[0, 0], c_recv.at[way, steps - 1], core).wait_recv()
    multiply(lax.rem(z + steps, nz))
    finish_step(steps - 2)
    finish(lax.rem(z + steps, nz))

    lane_at = lax.broadcasted_iota(jnp.int32, (half, 2 * roll), 1)
    streams = []
    for k in range(per):
        left, right = [
            turned[pl.ds(pl.multiple_of(shift + k * cols, 8), half), :] for shift in shifts
        ]
        streams.append(jnp.where(lane_at < roll, left, right))
    for source in range(4):
        mine = jnp.logical_and(yh == source, yh // 2 == yl)

        @pl.when(jnp.logical_not(mine))
        def _(source=source):
            remote(
                ysend.at[0, 0], ybuf.at[source], y_send.at[0, 0], y_recv.at[source], across
            ).wait_recv()

        for k in range(per):
            streams[k] += ybuf[source, k].astype(jnp.float32)
    stream = jnp.concatenate(streams, axis=0)

    square = jnp.sum(stream * stream, axis=0, keepdims=True)
    square = jnp.broadcast_to(square, (8, 2 * roll))
    square = square + pltpu.roll(square, roll, 1)
    ss_out[...] = square

    def s_copy(r):
        return remote(ss_out, ss_in.at[r - 1], s_send.at[0], s_recv.at[0], section[r - 1])

    for r in range(1, 16):
        s_copy(r).start()
    remote(ss_in, ss_in, s_send.at[0], s_recv.at[0], core).wait_recv()
    for r in range(1, 16):
        square += ss_in[r - 1]
    scale = lax.rsqrt(square * (1.0 / (16 * share)) + norm_eps)
    normed = (stream * scale[0:1]).T
    natural = []
    for k in range(per):
        for i in range(2):
            natural.append(normed[i * roll : (i + 1) * roll, k * half : (k + 1) * half])
    natural = jnp.concatenate(natural, axis=1)
    out_ref[...] = natural

    pair.wait_send()
    for slot in range(1, 4):
        for n in pieces:
            h_copy(slot, n).wait_send()

    def drain(ref, sem):
        remote(ref, ref, sem, p_recv.at[0], core).wait_send()

    for slot in range(3):
        drain(ot.at[0, :, 0], o_send.at[slot])
        drain(xbuf.at[slot], x_send.at[slot])
    drain(wall.at[0, 0], own_send.at[0])
    for way in range(2):
        for sub in range(2):
            count = steps if way == sub else steps - 1
            for sem in (r_send, w_send, c_send):
                drain(sbuf.at[way, sub, pl.ds(0, count)], sem.at[way, sub])
    for jj in range(2):
        for to_yl in range(2):
            mine = jnp.logical_and(yl == to_yl, yh == 2 * yl + jj)

            @pl.when(jnp.logical_not(mine))
            def _(to_yl=to_yl, jj=jj):
                spot = ysend.at[to_yl, jj]
                remote(spot, spot, y_send.at[to_yl, jj], y_recv.at[0], across).wait_send()

    drain(ss_in, s_send.at[0])


def update_and_decode(nz, hidden_act, out_grad, flat_in, state, resid):
    tokens, hidden = hidden_act.shape
    cols = state[0].shape[0]
    roll = flat_in.shape[0]
    steps = nz // 2
    per = 2 * nz // 8
    half = cols // 2
    share = per * cols
    span = (2 * cols + half + 112 + 127) // 128 * 128
    vmem = pl.BlockSpec(memory_space=pltpu.VMEM)
    hbm = pl.BlockSpec(memory_space=pl.ANY)
    dma = pltpu.SemaphoreType.DMA
    return pl.pallas_call(
        functools.partial(kernel, nz),
        out_shape=(
            jax.ShapeDtypeStruct((cols, hidden), jnp.float32),
            jax.ShapeDtypeStruct((roll, share), jnp.float32),
        ),
        in_specs=[hbm, hbm, hbm, [hbm] * 4, hbm],
        out_specs=(vmem, vmem),
        scratch_shapes=[
            pltpu.VMEM(hidden_act.shape, jnp.bfloat16),
            pltpu.VMEM(flat_in.shape, jnp.bfloat16),
            pltpu.VMEM(out_grad.shape, jnp.bfloat16),
            pltpu.VMEM((2, nz, 2, cols, tokens), jnp.bfloat16),
            pltpu.VMEM((4 * tokens, hidden), jnp.bfloat16),
            pltpu.VMEM((nz, cols, 4 * tokens), jnp.bfloat16),
            pltpu.VMEM((2, 2, cols, hidden), jnp.float32),
            pltpu.VMEM((2, 2, steps, cols // 2, hidden), jnp.bfloat16),
            pltpu.VMEM((2, 2, steps, cols // 2, hidden), jnp.bfloat16),
            pltpu.VMEM((4, cols, hidden), jnp.float32),
            pltpu.VMEM((2 * roll, hidden), jnp.bfloat16),
            pltpu.VMEM((nz, 2, cols, hidden), jnp.bfloat16),
            pltpu.VMEM((8, per, cols, 2 * roll), jnp.bfloat16),
            pltpu.VMEM((3, 2, per, cols, 2 * roll), jnp.bfloat16),
            pltpu.VMEM((2, 2, per, half, 2 * roll), jnp.bfloat16),
            pltpu.VMEM((4, per, half, 2 * roll), jnp.bfloat16),
            pltpu.VMEM((8, 2 * roll), jnp.float32),
            pltpu.VMEM((15, 8, 2 * roll), jnp.float32),
            pltpu.VMEM((2 * roll, span), jnp.bfloat16),
            pltpu.VMEM((span, 2 * roll), jnp.float32),
            dma((3, 2)),
            dma((3, 2)),
            dma((3,)),
            dma((nz,)),
            dma((2, 2)),
            dma((2, 2, 2, steps)),
            dma((11,)),
            dma((1,)),
            dma((1,)),
            dma((2, 2)),
            dma((2, 2, 2, steps)),
            dma((2, 2)),
            dma((2, steps)),
            dma((1,)),
            dma((1,)),
            dma((3,)),
            dma((2, per)),
            dma((2, 2)),
            dma((4,)),
            dma((1,)),
            dma((1,)),
        ],
        compiler_params=pltpu.CompilerParams(collective_id=0, has_side_effects=True),
        cost_estimate=pl.CostEstimate(
            flops=8 * nz * cols * hidden * (tokens + roll),
            bytes_accessed=3000000,
            transcendentals=0,
        ),
        name="update_and_decode",
    )(hidden_act, out_grad, flat_in, list(state), resid)


def per_device(
    hidden_act,
    out_grad,
    grad_accum,
    master_weight,
    adam_first,
    adam_second,
    decode_in,
    residual_in,
    norm_gain,
):
    nz = lax.axis_size("z")
    steps_count, roll_rows, hidden_local = decode_in.shape
    flat_rows = steps_count * roll_rows
    flat_in = decode_in.reshape(flat_rows, hidden_local)
    resid_flat = residual_in.reshape(flat_rows, -1)
    state = (grad_accum.T, master_weight.T, adam_first.T, adam_second.T)
    grad_share, normed = update_and_decode(
        nz, hidden_act, out_grad, flat_in, state, resid_flat
    )
    weight_new, first_new, second_new = new_weight(
        grad_share.T + grad_accum, master_weight, adam_first, adam_second
    )
    decoded = (normed * norm_gain.astype(jnp.float32)).astype(jnp.bfloat16)
    decoded = decoded.reshape(steps_count, roll_rows, -1)
    return (weight_new, first_new, second_new, decoded)


def solution(mesh):
    finer = Mesh(mesh.devices.reshape(2, 12, 2, 4, 4), ("yl", "z", "c", "yh", "x"))
    in_specs = (
        P(DP, SECTION),
        P(DP, None),
        P(SECTION, DP),
        P(SECTION, DP),
        P(SECTION, DP),
        P(SECTION, DP),
        P(None, DP, SECTION),
        P(None, DP, None),
        P(SECTION),
    )
    out_specs = (P(SECTION, DP), P(SECTION, DP), P(SECTION, DP), P(None, DP, SECTION))
    return jax.shard_map(
        per_device, mesh=finer, in_specs=in_specs, out_specs=out_specs, check_vma=False
    )
```
